512 devices in a mesh: seq: 64 (over z_lo, x, core), batch: 8 (over y, z_hi).
Axes of the slice: x: 4, y: 4, z: 16 (z_hi: 2, z_lo: 8; z = z_hi * 8 + z_lo), core: 2. Of those that a mesh axis runs over, the one named last changes fastest.
Arguments:
- activ: bfloat16 [8, 8192, 384], P('batch', 'seq'), may hold values from -6 to 6
- gain: float32 [384], replicated, may hold values from 0.1 to 1.9
- weight: bfloat16 [5, 384, 448], P(None, 'seq'), may hold values from -0.125 to 0.125
- bias: float32 [448], replicated, may hold values from -0.5 to 0.5
- cotangent: bfloat16 [8, 4096, 448], P('batch', 'seq'), may hold values from -6 to 6
Outputs:
- pooled: bfloat16 [8, 4096, 448], P('batch', 'seq')
- grad_input: bfloat16 [8, 8192, 384], P('batch', 'seq')
- grad_weight: float32 [5, 384, 448], P(None, 'seq')
- grad_gain: float32 [384], replicated
- grad_bias: float32 [448], replicated
The draws below stay inside these ranges and needn't reach their ends.
All inputs are finite; a program needn't handle non-finite values.
Results may differ from the reference program's by a relative error of at most 0.0043.
Values may be sent and summed in bfloat16 or wider, within the bound.
A program may use at most 64 MiB of HBM per device.

```python
import jax
import jax.numpy as jnp
from jax import lax

C_IN = 384
C_OUT = 448
KERNEL = 5
BATCH = 8
LENGTH = 8192
HALF = 4096


def steps_of(key, dims, shards, low, high):
    def one(position, shards_of):
        steps = jax.random.uniform(jax.random.fold_in(jax.random.fold_in(key, 6), position), (shards_of,), jnp.float32, low / len(shards), high / len(shards))
        return jnp.repeat(jnp.exp(steps), dims[position] // shards_of).reshape((-1,) + (1,) * (len(dims) - position - 1))

    factor_of = one(*shards[0])
    for cut in shards[1:]:
        factor_of = factor_of * one(*cut)
    return factor_of


def scatter_about(rng, shape, deviation, most, shards=(), dtype=jnp.bfloat16):
    drawn = deviation * jax.random.normal(rng, shape, jnp.float32)
    if shards:
        drawn = drawn * steps_of(rng, shape, shards, -0.22, 0.18)
    return jnp.clip(drawn, -most, most).astype(dtype)


def setup_inputs(seed: int = 0) -> dict:
    splits = jax.random.split(jax.random.key(seed), 6)
    return {
        "activ": scatter_about(splits[0], (BATCH, LENGTH, C_IN), 1.0, 6.0, ((0, 8), (1, 64))),
        "gain": jnp.clip(1.0 + 0.18 * jax.random.normal(splits[1], (C_IN,), jnp.float32), 0.1, 1.9),
        "weight": scatter_about(splits[2], (KERNEL, C_IN, C_OUT), (KERNEL * C_IN) ** -0.5, 0.125, ((1, 64),)),
        "bias": jnp.clip(jax.random.uniform(splits[3], (C_OUT,), jnp.float32, -0.5, 0.5), -0.5, 0.5),
        "cotangent": scatter_about(splits[4], (BATCH, HALF, C_OUT), 1.0, 6.0, ((0, 8), (1, 64))),
    }


def one_sequence(inputs, gain, weight, bias, cot_rows):
    scaled = inputs.astype(jnp.float32) * gain
    activated, gelu_back = jax.vjp(jax.nn.gelu, scaled)
    activated = activated.astype(jnp.bfloat16)
    padded = jnp.pad(activated, ((2, 2), (0, 0)))
    conv_out = jnp.zeros((LENGTH, C_OUT), jnp.float32) + bias
    for offset in range(KERNEL):
        conv_out = conv_out + jnp.dot(padded[offset:offset + LENGTH], weight[offset], preferred_element_type=jnp.float32)
    paired = conv_out.reshape(LENGTH // 2, 2, C_OUT)
    pooled = (0.5 * (paired[:, 0] + paired[:, 1])).astype(jnp.bfloat16)
    grad_conv = (0.5 * jnp.repeat(cot_rows.astype(jnp.float32), 2, axis=0)).astype(jnp.bfloat16)
    grad_padded = jnp.pad(grad_conv, ((2, 2), (0, 0)))
    grad_act = jnp.zeros((LENGTH, C_IN), jnp.float32)
    for offset in range(KERNEL):
        grad_act = grad_act + jnp.dot(grad_padded[4 - offset:4 - offset + LENGTH], weight[offset].T, preferred_element_type=jnp.float32)
    weight_part = jnp.stack([jnp.dot(padded[offset:offset + LENGTH].T, grad_conv, preferred_element_type=jnp.float32) for offset in range(KERNEL)], axis=0)
    grad_pre = gelu_back(grad_act)[0]
    grad_input = (grad_pre * gain).astype(jnp.bfloat16)
    gain_part = lax.optimization_barrier(jnp.sum(grad_pre * inputs.astype(jnp.float32), axis=0))
    bias_part = lax.optimization_barrier(jnp.sum(grad_conv.astype(jnp.float32), axis=0))
    return (pooled, grad_input, weight_part, gain_part, bias_part)

def reference(activ, gain, weight, bias, cotangent):

    def single(pair):
        return one_sequence(pair[0], gain, weight, bias, pair[1])
    pooled, grad_input, weight_parts, gain_parts, bias_parts = lax.map(single, (activ, cotangent))
    factor = float(BATCH * LENGTH) ** (-0.5)
    grad_weight = lax.optimization_barrier(jnp.sum(weight_parts, axis=0)) * factor
    grad_gain = lax.optimization_barrier(jnp.sum(gain_parts, axis=0)) * factor
    grad_bias = lax.optimization_barrier(jnp.sum(bias_parts, axis=0)) * factor
    return (pooled, grad_input, grad_weight, grad_gain, grad_bias)
```

```python
import dataclasses
import functools

import jax
import jax.numpy as jnp
from jax import lax
from jax.experimental import pallas as pl
from jax.experimental.pallas import tpu as pltpu
from jax.sharding import PartitionSpec as P

MESH = pl.DeviceIdType.MESH
F32 = jnp.float32
BF16 = jnp.bfloat16
HI = lax.Precision.HIGHEST
ROOT = 0.7978845608028654
CUBE = 0.044715
PAD = 8


@dataclasses.dataclass(frozen=True)
class Plan:
    nx: int = 4
    ny: int = 4
    nzl: int = 8
    nzh: int = 2
    own: int = 6
    taps: int = 5
    rows: int = 128
    cout: int = 448

    @property
    def nz(self):
        return self.nzl * self.nzh

    @property
    def cin(self):
        return self.own * self.nzl * self.nx * 2

    @property
    def block(self):
        return self.own * self.nzl

    @property
    def half(self):
        return self.block * self.nx

    @property
    def halfp(self):
        return -(-self.half // 128) * 128

    @property
    def coutp(self):
        return self.ny * 128

    @property
    def offsets(self):
        far = self.nzl // 2
        return tuple(range(1, far + 1)) + tuple(-o for o in range(1, self.nzl - far))


def dot(a, b, dims, precision=None):
    return lax.dot_general(a, b, (dims, ((), ())), precision=precision, preferred_element_type=F32)


NN = ((1,), (0,))
NT = ((1,), (1,))
TN = ((0,), (0,))


def kernel(
    plan, factor,
    activ, gain, weight, bias, cot,
    pooled, grad_input, grad_weight, grad_gain, grad_bias,
    act_p, cot_p, act_h, cot_h, sel, af, gf, ct, zb, wf, wx, dws, dwo, yr, xs, xo, xr, zo, zs, zr, ya,
    cks, io, gi_s, gi_r, pf_s, pf_r, gx, gt, gy, gs, gz,
    s_loc, r_loc, s_az, r_az, s_ax, r_ax, s_y, r_y, s_x, r_x, s_z, r_z, s_ya, r_ya, s_gx, r_gx, s_gy, r_gy, s_gz, r_gz,
):
    p = plan
    nx, ny, nz, nzl = p.nx, p.ny, p.nz, p.nzl
    rows, half, block, own, taps = p.rows, p.half, p.block, p.own, p.taps
    pairs = rows // 2
    seq, batch = lax.axis_index("seq"), lax.axis_index("batch")
    core = seq % 2
    x = (seq // 2) % nx
    z_lo = seq // (2 * nx)
    z_hi = batch % p.nzh
    y = batch // p.nzh
    z = z_hi * nzl + z_lo
    sign = 1 - 2 * core
    other = 1 - core

    def device(zz, xx, cc, yy):
        return ((zz % nzl) * (2 * nx) + xx * 2 + cc, yy * p.nzh + zz // nzl)

    def at_z(d):
        return (z + d + nz) % nz

    def at_x(d):
        return (x + d) % nx

    def at_y(d):
        return (y + d) % ny

    chip = z * nx + x
    chips = nz * nx
    nxt = (chip + 1) % chips
    prv = (chip + chips - 1) % chips

    partner = device(z, x, other, y)

    def chip_core(c, cc):
        return device(c // nx, c % nx, cc, y)

    barrier = pltpu.get_barrier_semaphore()
    peers = [partner]
    peers += [device(z, at_x(d), cc, y) for d in range(1, nx) for cc in (core, other)]
    peers += [device(z, x, core, at_y(d)) for d in range(1, ny)]
    far = nzl // 2
    peers += [device(at_z(s * o), x, core, y) for o in range(1, far + 1) for s in (1, -1)]
    peers += [chip_core(c, cc) for c in (nxt, prv) for cc in (0, 1)]
    for peer in peers:
        pl.semaphore_signal(barrier, inc=1, device_id=peer, device_id_type=MESH)

    q = lax.broadcasted_iota(jnp.int32, (p.cin, p.halfp), 1)
    r = lax.broadcasted_iota(jnp.int32, (p.cin, p.halfp), 0)
    chan = own * ((q % block) // own * (2 * nx) + (q // block) * 2) + q % own
    valid = q < half
    sel[0] = jnp.where(valid & (r == chan), 1.0, 0.0).astype(BF16)
    sel[1] = jnp.where(valid & (r == chan + own), 1.0, 0.0).astype(BF16)
    mine = sel[core]

    ct[...] = jnp.zeros_like(ct)
    tiles = p.halfp // 128

    def put(start, value):
        for t in range(tiles):
            af[t, pl.ds(start, value.shape[0]), :] = value[:, 128 * t:128 * t + 128]

    put(pl.multiple_of(PAD + rows * core, 8), dot(activ[0], mine, NN))
    ct[pl.ds(pl.multiple_of(PAD + pairs * core, 8), pairs), 0:p.cout] = cot[0].astype(F32)
    gain_half = dot(jnp.broadcast_to(gain[...], (8, p.cin)), mine.astype(F32), NN, HI)[0:1]

    pl.semaphore_wait(barrier, len(peers))

    started = []

    def send(src, dst, s, r_, to):
        copy = pltpu.make_async_remote_copy(
            src_ref=src, dst_ref=dst, send_sem=s, recv_sem=r_, device_id=to, device_id_type=MESH
        )
        copy.start()
        started.append(copy)
        return copy

    c_act = send(activ.at[0], act_p, s_loc.at[0], r_loc.at[0], partner)
    c_cot = send(cot.at[0], cot_p, s_loc.at[1], r_loc.at[1], partner)
    edge = 16
    up_chip = jnp.where(core == 1, nxt, prv)
    side = core
    halos = []
    a_edge = pl.ds(pl.multiple_of(core * (rows - edge), edge), edge)
    c_edge = pl.ds(pl.multiple_of(core * (pairs - edge), edge), edge)
    for i, cc in enumerate((0, 1)):
        to = chip_core(up_chip, cc)
        halos.append(send(activ.at[0, a_edge], act_h.at[side], s_loc.at[2 + i], r_loc.at[2 + side], to))
        halos.append(send(cot.at[0, c_edge], cot_h.at[side], s_loc.at[4 + i], r_loc.at[4 + side], to))
    c_az = []
    for i, o in enumerate(p.offsets):
        to = device(at_z(sign * o), x, core, y)
        c_az.append(send(weight, zb.at[z_lo], s_az.at[i], r_az.at[i], to))
    zb[z_lo] = weight[...]

    c_act.wait_recv()
    put(pl.multiple_of(PAD + rows * other, 8), dot(act_p[...], mine, NN))
    c_cot.wait_recv()
    ct[pl.ds(pl.multiple_of(PAD + pairs * other, 8), pairs), 0:p.cout] = cot_p[...].astype(F32)
    for s in (0, 1):
        for src, dst, i in ((activ.at[0, a_edge], act_h, 2), (cot.at[0, c_edge], cot_h, 4)):
            pltpu.make_async_remote_copy(
                src_ref=src, dst_ref=dst.at[s], send_sem=s_loc.at[i], recv_sem=r_loc.at[i + s],
                device_id=partner, device_id_type=MESH,
            ).wait_recv()
    place = z_lo * nx + x
    before = jnp.where(place > 0, 1.0, 0.0).astype(F32)
    after = jnp.where(place < nzl * nx - 1, 1.0, 0.0).astype(F32)
    put(0, (dot(act_h[1], mine, NN) * before)[edge - PAD:edge])
    put(PAD + 2 * rows, (dot(act_h[0], mine, NN) * after)[0:PAD])
    ct[0:PAD, 0:p.cout] = (cot_h[1].astype(F32) * before)[edge - PAD:edge]
    ct[PAD + rows:, 0:p.cout] = (cot_h[0].astype(F32) * after)[0:PAD]

    for t in range(tiles):
        v = af[t] * gain_half[:, 128 * t:128 * t + 128]
        gf[t] = (0.5 * v * (1.0 + jnp.tanh(ROOT * (v + CUBE * v * v * v)))).astype(BF16).astype(F32)

    def strided(ref, start):
        return jnp.concatenate(
            [ref[t, pl.ds(start, rows, 2), :] for t in range(tiles)], axis=1
        )

    shifted = [strided(gf, PAD - 2 + j).astype(BF16) for j in range(taps + 1)]
    cots = [ct[PAD + d:PAD + d + rows, :].astype(BF16) for d in (-1, 0, 1)]

    even, odd = shifted[2], shifted[3]
    se = [dot(even, c, TN)[0:half] for c in cots]
    so = [dot(odd, c, TN)[0:half] for c in cots]
    for k, (e, o) in enumerate(((2, 2), (1, 2), (1, 1), (0, 1), (0, 0))):
        part = 0.5 * (se[e] + so[o])
        for t in range(ny):
            dwo[t, k] = part[:, 128 * t:128 * t + 128]
            dws[t, k] = part[:, 128 * t:128 * t + 128].astype(BF16)
    c_y = []
    for d in range(1, ny):
        c_y.append(send(dws.at[at_y(d)], yr.at[d - 1], s_y.at[d - 1], r_y.at[d - 1], device(z, x, core, at_y(d))))

    for c in c_az:
        c.wait_recv()
    for k in range(taps):
        for zz in range(nzl):
            wf[own * zz:own * (zz + 1)] = zb[zz, k].astype(F32)
        wx[x, k] = wf[...].astype(BF16)
    c_ax = []
    for d in range(1, nx):
        c_ax.append(send(wx.at[x], wx.at[x], s_ax.at[d - 1], r_ax.at[d - 1], device(z, at_x(d), core, y)))

    for c in c_y:
        c.wait_recv()
    for k in range(taps):
        total = dwo[y, k]
        for d in range(ny - 1):
            total = total + yr[d, k].astype(F32)
        for xx in range(nx):
            piece = total[block * xx:block * (xx + 1)]
            xo[xx, k] = piece
            xs[xx, k] = piece.astype(BF16)
    c_x = []
    for d in range(1, nx):
        c_x.append(send(xs.at[at_x(d)], xr.at[d - 1], s_x.at[d - 1], r_x.at[d - 1], device(z, at_x(d), core, y)))

    for c in c_ax:
        c.wait_recv()
    conv = jnp.zeros((rows, p.cout), F32)
    cot_all = ct[:, 0:p.cout].astype(BF16)
    for k in range(taps):
        w = wx[:, k].reshape(half, p.cout)
        conv = conv + dot(shifted[k][:, 0:half], w, NN)
        conv = conv + dot(shifted[k + 1][:, 0:half], w, NN)
        cks[k, :, 0:half] = dot(cot_all, w, NT)
        if half < p.halfp:
            cks[k, :, half:] = jnp.zeros((rows + 2 * PAD, p.halfp - half), F32)
    conv = 0.5 * conv
    for h in (0, 1):
        pf_s[h] = conv[pairs * h:pairs * (h + 1)]
    c_pf = send(pf_s.at[other], pf_r, s_loc.at[6], r_loc.at[6], partner)

    def shift(k, d):
        return cks[k, PAD + d:PAD + d + rows, :]

    grad_even = 0.5 * (shift(0, 1) + shift(1, 0) + shift(2, 0) + shift(3, -1) + shift(4, -1))
    grad_odd = 0.5 * (shift(0, 1) + shift(1, 1) + shift(2, 0) + shift(3, 0) + shift(4, -1))
    gain_part = jnp.zeros((1, p.halfp), F32)
    for start, grad in ((0, grad_even), (1, grad_odd)):
        a = strided(af, PAD + start)
        v = a * gain_half
        t = jnp.tanh(ROOT * (v + CUBE * v * v * v))
        slope = 0.5 * (1.0 + t) + 0.5 * v * (1.0 - t * t) * (ROOT * (1.0 + 3.0 * CUBE * v * v))
        pre = grad * slope
        gain_part = gain_part + jnp.sum(pre * a, axis=0, keepdims=True)
        out = pre * gain_half
        for tt in range(p.halfp // 128):
            io[tt, pl.ds(start, rows, 2), :] = out[:, 128 * tt:128 * tt + 128]
    for h in (0, 1):
        gi_s[h] = jnp.concatenate(
            [io[tt, rows * h:rows * (h + 1), :] for tt in range(p.halfp // 128)], axis=1
        ).astype(BF16)
    c_gi = send(gi_s.at[other], gi_r, s_loc.at[7], r_loc.at[7], partner)

    gt[...] = jnp.zeros_like(gt)
    for t in range(tiles):
        gt[0, t:t + 1, :] = gain_part[:, 128 * t:128 * t + 128]
    bias_part = jnp.sum(ct[pl.ds(pl.multiple_of(PAD + pairs * core, 8), pairs), :], axis=0, keepdims=True)
    for t in range(ny):
        gt[0, 4 + t:5 + t, :] = bias_part[:, 128 * t:128 * t + 128]
    c_gx = []
    for flip in (0, 1):
        for d in range(nx):
            if flip == 0 and d == 0:
                continue
            i = flip * nx + d
            cc = core if flip == 0 else other
            c_gx.append(send(gt.at[0], gx.at[i], s_gx.at[i], r_gx.at[i], device(z, at_x(d), cc, y)))

    for c in c_x:
        c.wait_recv()
    zo[...] = jnp.zeros_like(zo)
    for k in range(taps):
        wf2 = xo[x, k]
        for d in range(nx - 1):
            wf2 = wf2 + xr[d, k].astype(F32)
        for zz in range(nzl):
            zo[zz, own * k:own * (k + 1), :] = wf2[own * zz:own * (zz + 1)]
    zs[...] = zo[...].astype(BF16)
    c_z = []
    for d in range(1, nz):
        c_z.append(send(zs.at[at_z(d) % nzl], zr.at[d - 1], s_z.at[d - 1], r_z.at[d - 1], device(at_z(d), x, core, y)))

    for c in c_gx:
        c.wait_recv()
    same = gt[0]
    for d in range(1, nx):
        same = same + gx[d]
    flipped = gx[nx]
    for d in range(1, nx):
        flipped = flipped + gx[nx + d]
    first = jnp.where(core == 0, same, flipped)
    second = jnp.where(core == 0, flipped, same)
    gt[1, 0:2, :] = first[0:2]
    gt[1, 2:4, :] = second[0:2]
    gt[1, 4:8, :] = (first + second)[4:8]
    c_gy = []
    for d in range(1, ny):
        c_gy.append(send(gt.at[1], gy.at[d - 1], s_gy.at[d - 1], r_gy.at[d - 1], device(z, x, core, at_y(d))))
    for c in c_gy:
        c.wait_recv()
    total = gt[1]
    for d in range(ny - 1):
        total = total + gy[d]
    gs[...] = total
    c_gz = []
    for d in range(1, nz):
        c_gz.append(send(gs, gz.at[d - 1], s_gz.at[d - 1], r_gz.at[d - 1], device(at_z(d), x, core, y)))

    c_pf.wait_recv()
    pooled[0] = (pf_s[core] + pf_r[...] + bias[...]).astype(BF16)
    c_gi.wait_recv()
    grad_input[0] = (dot(gi_s[core], mine, NT) + dot(gi_r[...], sel[other], NT)).astype(BF16)

    for c in c_z:
        c.wait_recv()
    final = zo[z_lo]
    for d in range(nz - 1):
        final = final + zr[d].astype(F32)
    ya[y] = final * factor
    c_ya = []
    for d in range(1, ny):
        c_ya.append(send(ya.at[y], ya.at[y], s_ya.at[d - 1], r_ya.at[d - 1], device(z, x, core, at_y(d))))

    for c in c_gz:
        c.wait_recv()
    total = gs[...]
    for d in range(nz - 1):
        total = total + gz[d]
    total = total * factor
    halves = [
        jnp.concatenate([total[2 * h + t:2 * h + t + 1] for t in range(tiles)], axis=1) for h in (0, 1)
    ]
    summed = jnp.zeros((8, p.cin), F32)
    for h in (0, 1):
        wide = jnp.broadcast_to(halves[h], (8, p.halfp))
        summed = summed + dot(wide, sel[h].astype(F32), NT, HI)
    grad_gain[...] = summed[0:1]
    grad_bias[...] = jnp.concatenate([total[4 + t:5 + t] for t in range(ny)], axis=1)[:, 0:p.cout]

    for c in c_ya:
        c.wait_recv()
    for k in range(taps):
        wide = jnp.concatenate([ya[t, own * k:own * (k + 1), :] for t in range(ny)], axis=1)
        grad_weight[k] = wide[:, 0:p.cout]
    for c in started:
        c.wait_send()


def build(mesh, plan, factor):
    p = plan
    nx, ny, nz, nzl = p.nx, p.ny, p.nz, p.nzl
    pairs = p.rows // 2
    zrows = -(-p.own * p.taps // 16) * 16
    dma = pltpu.SemaphoreType.DMA
    sems = (8, len(p.offsets), nx - 1, ny - 1, nx - 1, nz - 1, ny - 1, 2 * nx, ny - 1, nz - 1)
    scratch = [
        pltpu.VMEM((p.rows, p.cin), BF16),
        pltpu.VMEM((pairs, p.cout), BF16),
        pltpu.VMEM((2, 16, p.cin), BF16),
        pltpu.VMEM((2, 16, p.cout), BF16),
        pltpu.VMEM((2, p.cin, p.halfp), BF16),
        pltpu.VMEM((p.halfp // 128, 2 * p.rows + 2 * PAD, 128), F32),
        pltpu.VMEM((p.halfp // 128, 2 * p.rows + 2 * PAD, 128), F32),
        pltpu.VMEM((p.rows + 2 * PAD, p.coutp), F32),
        pltpu.VMEM((nzl, p.taps, p.own, p.cout), BF16),
        pltpu.VMEM((p.block, p.cout), F32),
        pltpu.VMEM((nx, p.taps, p.block, p.cout), BF16),
        pltpu.VMEM((ny, p.taps, p.half, 128), BF16),
        pltpu.VMEM((ny, p.taps, p.half, 128), F32),
        pltpu.VMEM((ny - 1, p.taps, p.half, 128), BF16),
        pltpu.VMEM((nx, p.taps, p.block, 128), BF16),
        pltpu.VMEM((nx, p.taps, p.block, 128), F32),
        pltpu.VMEM((nx - 1, p.taps, p.block, 128), BF16),
        pltpu.VMEM((nzl, zrows, 128), F32),
        pltpu.VMEM((nzl, zrows, 128), BF16),
        pltpu.VMEM((nz - 1, zrows, 128), BF16),
        pltpu.VMEM((ny, zrows, 128), F32),
        pltpu.VMEM((p.taps, p.rows + 2 * PAD, p.halfp), F32),
        pltpu.VMEM((p.halfp // 128, 2 * p.rows, 128), F32),
        pltpu.VMEM((2, p.rows, p.halfp), BF16),
        pltpu.VMEM((p.rows, p.halfp), BF16),
        pltpu.VMEM((2, pairs, p.cout), F32),
        pltpu.VMEM((pairs, p.cout), F32),
        pltpu.VMEM((2 * nx, 8, 128), F32),
        pltpu.VMEM((2, 8, 128), F32),
        pltpu.VMEM((ny - 1, 8, 128), F32),
        pltpu.VMEM((8, 128), F32),
        pltpu.VMEM((nz - 1, 8, 128), F32),
    ]
    for n in sems:
        scratch += [dma((n,)), dma((n,))]
    vmem = pl.BlockSpec(memory_space=pltpu.VMEM)

    def per_device(activ, gain, weight, bias, cotangent):
        outs = pl.pallas_call(
            functools.partial(kernel, p, factor),
            out_shape=(
                jax.ShapeDtypeStruct((1, pairs, p.cout), BF16),
                jax.ShapeDtypeStruct((1, p.rows, p.cin), BF16),
                jax.ShapeDtypeStruct((p.taps, p.own, p.cout), F32),
                jax.ShapeDtypeStruct((1, p.cin), F32),
                jax.ShapeDtypeStruct((1, p.cout), F32),
            ),
            in_specs=[vmem] * 5,
            out_specs=(vmem,) * 5,
            scratch_shapes=scratch,
            compiler_params=pltpu.CompilerParams(collective_id=0, has_side_effects=True),
        )(activ, gain.reshape(1, -1), weight, bias.reshape(1, -1), cotangent)
        return (*outs[:3], outs[3].reshape(-1), outs[4].reshape(-1))

    in_specs = (P("batch", "seq", None), P(), P(None, "seq", None), P(), P("batch", "seq", None))
    out_specs = (P("batch", "seq", None), P("batch", "seq", None), P(None, "seq", None), P(), P())
    return jax.shard_map(per_device, mesh=mesh, in_specs=in_specs, out_specs=out_specs, check_vma=False)


def solution(mesh):
    return build(mesh, Plan(), float(8 * 8192) ** -0.5)
```

```python
import dataclasses
import functools

import jax
import jax.numpy as jnp
from jax import lax
from jax.experimental import pallas as pl
from jax.experimental.pallas import tpu as pltpu
from jax.sharding import PartitionSpec as P

MESH = pl.DeviceIdType.MESH
F32 = jnp.float32
BF16 = jnp.bfloat16
ROOT = 0.7978845608028654
CUBE = 0.044715
PAD = 8


@dataclasses.dataclass(frozen=True)
class Plan:
    nx: int = 4
    ny: int = 4
    nzl: int = 8
    nzh: int = 2
    own: int = 6
    taps: int = 5
    rows: int = 128
    cout: int = 448

    @property
    def nz(self):
        return self.nzl * self.nzh

    @property
    def cin(self):
        return self.own * self.nzl * self.nx * 2

    @property
    def block(self):
        return self.own * self.nzl

    @property
    def half(self):
        return self.block * self.nx

    @property
    def halfp(self):
        return -(-self.half // 128) * 128

    @property
    def coutp(self):
        return self.ny * 128

    @property
    def offsets(self):
        far = self.nzl // 2
        return tuple(range(1, far + 1)) + tuple(-o for o in range(1, self.nzl - far))


def dot(a, b, dims):
    return lax.dot_general(a, b, (dims, ((), ())), preferred_element_type=F32)


def picked(row, ones, dims):
    first = row.astype(BF16)
    rest = row - first.astype(F32)
    second = rest.astype(BF16)
    third = (rest - second.astype(F32)).astype(BF16)
    pieces = [jnp.broadcast_to(v.astype(F32), (8, row.shape[1])) for v in (first, second, third)]
    line = lax.broadcasted_iota(jnp.int32, pieces[0].shape, 0)
    rows = jnp.where(line == 0, pieces[0], jnp.where(line == 1, pieces[1], jnp.where(line == 2, pieces[2], 0.0)))
    out = dot(rows.astype(BF16), ones, dims)
    return out[0:1] + out[1:2] + out[2:3]


NN = ((1,), (0,))
NT = ((1,), (1,))
TN = ((0,), (0,))


TAPS = (2, 1, 3, 0, 4)
GROUPS = ((0, 16, (2, 1)), (16, 16, (3, 0)), (32, 8, (4,)))
ORDER = (
    ("wz", 0), ("wz", 1), ("wz", 2), ("ys", 0), ("wz", 3), ("wz", 4), ("cv", 0), ("ys", 1), ("cv", 1), ("ys", 2),
    ("cv", 2), ("xs", 0), ("ys", 3), ("cv", 3), ("ys", 4), ("cv", 4),
)
LATE = (1, 2)


def kernel(
    plan, factor,
    activ, gain, weight, bias, cot,
    pooled, grad_input, grad_weight, grad_gain, grad_bias,
    act_p, cot_p, act_h, cot_h, sel, af, gf, ct, zb, wf, wx, dws, dwo, yr, xs, xo, xr, zo, zs0, zs1, zs2, zr0, zr1, zr2, ya,
    cks, io, gi_s, gi_r, pf_s, pf_r, gx, gt, gs, gz,
    s_loc, r_loc, s_az, r_az, s_ax, r_ax, s_y, r_y, s_x, r_x, s_z, r_z, s_ya, r_ya, s_gx, r_gx, s_gz, r_gz,
):
    p = plan
    nx, ny, nz, nzl = p.nx, p.ny, p.nz, p.nzl
    rows, half, block, own, taps = p.rows, p.half, p.block, p.own, p.taps
    pairs = rows // 2
    seq, batch = lax.axis_index("seq"), lax.axis_index("batch")
    core = seq % 2
    x = (seq // 2) % nx
    z_lo = seq // (2 * nx)
    z_hi = batch % p.nzh
    y = batch // p.nzh
    z = z_hi * nzl + z_lo
    sign = 1 - 2 * core
    other = 1 - core

    def device(zz, xx, cc, yy):
        return ((zz % nzl) * (2 * nx) + xx * 2 + cc, yy * p.nzh + zz // nzl)

    def at_z(d):
        return (z + d + nz) % nz

    def at_x(d):
        return (x + d) % nx

    def at_y(d):
        return (y + d) % ny

    chip = z * nx + x
    chips = nz * nx
    nxt = (chip + 1) % chips
    prv = (chip + chips - 1) % chips

    partner = device(z, x, other, y)

    def chip_core(c, cc):
        return device(c // nx, c % nx, cc, y)

    barrier = pltpu.get_barrier_semaphore()
    peers = [partner]
    peers += [device(z, at_x(d), cc, y) for d in range(1, nx) for cc in (core, other)]
    peers += [device(z, x, core, at_y(d)) for d in range(1, ny)]
    far = nzl // 2
    peers += [device(at_z(s * o), x, core, y) for o in range(1, far + 1) for s in (1, -1)]
    peers += [chip_core(c, cc) for c in (nxt, prv) for cc in (0, 1)]
    for peer in peers:
        pl.semaphore_signal(barrier, inc=1, device_id=peer, device_id_type=MESH)

    q = lax.broadcasted_iota(jnp.int32, (8, p.halfp), 1)
    chan = own * ((q % block) // own * (2 * nx) + (q // block) * 2) + q % own
    chan = jnp.where(q < half, chan, 2 * p.cin)[0:1]
    r = lax.broadcasted_iota(jnp.int32, (p.cin, p.halfp), 0)
    sel[0] = jnp.where(r == chan, 1.0, 0.0).astype(BF16)
    sel[1] = jnp.where(r == chan + own, 1.0, 0.0).astype(BF16)
    mine = sel[core]

    ct[...] = jnp.zeros_like(ct)
    tiles = p.halfp // 128

    def put(start, value):
        for t in range(tiles):
            af[t, pl.ds(start, value.shape[0]), :] = value[:, 128 * t:128 * t + 128]

    put(pl.multiple_of(PAD + rows * core, 8), dot(activ[0], mine, NN))
    ct[pl.ds(pl.multiple_of(PAD + pairs * core, 8), pairs), 0:p.cout] = cot[0].astype(F32)
    gain_half = picked(gain[...], mine, NN)

    pl.semaphore_wait(barrier, len(peers))

    started = []

    def send(src, dst, s, r_, to):
        copy = pltpu.make_async_remote_copy(
            src_ref=src, dst_ref=dst, send_sem=s, recv_sem=r_, device_id=to, device_id_type=MESH
        )
        copy.start()
        started.append(copy)
        return copy

    c_act = send(activ.at[0], act_p, s_loc.at[0], r_loc.at[0], partner)
    c_cot = send(cot.at[0], cot_p, s_loc.at[1], r_loc.at[1], partner)
    edge = 16
    up_chip = jnp.where(core == 1, nxt, prv)
    side = core
    halos = []
    a_edge = pl.ds(pl.multiple_of(core * (rows - edge), edge), edge)
    c_edge = pl.ds(pl.multiple_of(core * (pairs - edge), edge), edge)
    for i, cc in enumerate((0, 1)):
        to = chip_core(up_chip, cc)
        halos.append(send(activ.at[0, a_edge], act_h.at[side], s_loc.at[2 + i], r_loc.at[2 + side], to))
        halos.append(send(cot.at[0, c_edge], cot_h.at[side], s_loc.at[4 + i], r_loc.at[4 + side], to))
    n_off = len(p.offsets)
    c_az = []
    for k in range(taps):
        for i, o in enumerate(p.offsets):
            j = k * n_off + i
            c_az.append(send(weight.at[k], zb.at[z_lo, k], s_az.at[j], r_az.at[j], device(at_z(sign * o), x, core, y)))
    zb[z_lo] = weight[...]

    def activate(start, count):
        for t in range(tiles):
            v = af[t, start:start + count, :] * gain_half[:, 128 * t:128 * t + 128]
            gf[t, start:start + count, :] = (
                0.5 * v * (1.0 + jnp.tanh(ROOT * (v + CUBE * v * v * v)))
            ).astype(BF16).astype(F32)

    def strided(ref, start):
        return jnp.concatenate([ref[t, pl.ds(start, rows, 2), :] for t in range(tiles)], axis=1)

    def cot_shift(d):
        return ct[PAD + d:PAD + d + rows, :].astype(BF16)

    c_y = [None] * taps

    def y_send(k, part):
        for t in range(ny):
            dwo[t, k] = part[:, 128 * t:128 * t + 128]
            dws[t, k] = part[:, 128 * t:128 * t + 128].astype(BF16)
        c_y[k] = []
        for d in range(1, ny):
            i = (ny - 1) * k + d - 1
            c_y[k].append(send(dws.at[at_y(d), k], yr.at[d - 1, k], s_y.at[i], r_y.at[i], device(z, x, core, at_y(d))))

    c_act.wait_recv()
    put(pl.multiple_of(PAD + rows * other, 8), dot(act_p[...], mine, NN))
    c_cot.wait_recv()
    ct[pl.ds(pl.multiple_of(PAD + pairs * other, 8), pairs), 0:p.cout] = cot_p[...].astype(F32)
    activate(PAD, 2 * rows)
    even, odd = strided(gf, PAD).astype(BF16), strided(gf, PAD + 1).astype(BF16)
    here = cot_shift(0)
    e0, o0 = dot(even, here, TN)[0:half], dot(odd, here, TN)[0:half]
    y_send(2, 0.5 * (e0 + o0))

    for s in (0, 1):
        for src, dst, i in ((activ.at[0, a_edge], act_h, 2), (cot.at[0, c_edge], cot_h, 4)):
            pltpu.make_async_remote_copy(
                src_ref=src, dst_ref=dst.at[s], send_sem=s_loc.at[i], recv_sem=r_loc.at[i + s],
                device_id=partner, device_id_type=MESH,
            ).wait_recv()
    place = z_lo * nx + x
    before = jnp.where(place > 0, 1.0, 0.0).astype(F32)
    after = jnp.where(place < nzl * nx - 1, 1.0, 0.0).astype(F32)
    ct[0:PAD, 0:p.cout] = (cot_h[1].astype(F32) * before)[edge - PAD:edge]
    ct[PAD + rows:, 0:p.cout] = (cot_h[0].astype(F32) * after)[0:PAD]
    up, down = cot_shift(1), cot_shift(-1)
    o_up = dot(odd, up, TN)[0:half]
    y_send(1, 0.5 * (e0 + o_up))
    e_down = dot(even, down, TN)[0:half]
    y_send(3, 0.5 * (e_down + o0))
    y_send(0, 0.5 * (dot(even, up, TN)[0:half] + o_up))
    y_send(4, 0.5 * (e_down + dot(odd, down, TN)[0:half]))
    put(0, (dot(act_h[1], mine, NN) * before)[edge - PAD:edge])
    put(PAD + 2 * rows, (dot(act_h[0], mine, NN) * after)[0:PAD])
    activate(0, PAD)
    activate(PAD + 2 * rows, PAD)

    c_ax = []

    def weights_z(k):
        for c in c_az[n_off * k:n_off * (k + 1)]:
            c.wait_recv()
        for zz in range(nzl):
            wf[k % 2, own * zz:own * (zz + 1)] = zb[zz, k].astype(F32)
        wx[x, k] = wf[k % 2].astype(BF16)
        for d in range(1, nx):
            i = (nx - 1) * k + d - 1
            c_ax.append(send(wx.at[x, k], wx.at[x, k], s_ax.at[i], r_ax.at[i], device(z, at_x(d), core, y)))

    c_x = {}

    def y_sum(n):
        k = TAPS[n]
        for c in c_y[k]:
            c.wait_recv()
        total = dwo[y, k]
        for d in range(ny - 1):
            total = total + yr[d, k].astype(F32)
        for xx in range(nx):
            piece = total[block * xx:block * (xx + 1)]
            xo[xx, k] = piece
            xs[xx, k] = piece.astype(BF16)
        c_x[k] = []
        for d in range(1, nx):
            i = (nx - 1) * k + d - 1
            c_x[k].append(send(xs.at[at_x(d), k], xr.at[d - 1, k], s_x.at[i], r_x.at[i], device(z, at_x(d), core, y)))

    z_s, z_r = (zs0, zs1, zs2), (zr0, zr1, zr2)
    c_z = []

    def x_sum(g):
        base, length, members = GROUPS[g]
        zo[:, base:base + length, :] = jnp.zeros((nzl, length, 128), F32)
        for n, k in enumerate(members):
            for c in c_x[k]:
                c.wait_recv()
            total = xo[x, k]
            for d in range(nx - 1):
                total = total + xr[d, k].astype(F32)
            for zz in range(nzl):
                zo[zz, base + own * n:base + own * (n + 1), :] = total[own * zz:own * (zz + 1)]
        z_s[g][...] = zo[:, base:base + length, :].astype(BF16)
        for d in range(1, nz):
            i = (nz - 1) * g + d - 1
            c_z.append(
                send(z_s[g].at[at_z(d) % nzl], z_r[g].at[d - 1], s_z.at[i], r_z.at[i], device(at_z(d), x, core, y))
            )

    acc = [None]
    cot_all = ct[:, 0:p.cout].astype(BF16)
    shifted = [strided(gf, PAD - 2 + j)[:, 0:half].astype(BF16) for j in range(taps + 1)]

    def convs(k):
        for c in c_ax[(nx - 1) * k:(nx - 1) * (k + 1)]:
            c.wait_recv()
        w = wx[:, k].reshape(half, p.cout)
        add = dot(shifted[k], w, NN) + dot(shifted[k + 1], w, NN)
        acc[0] = add if acc[0] is None else acc[0] + add
        cks[k, :, 0:half] = dot(cot_all, w, NT)
        if half < p.halfp:
            cks[k, :, half:] = jnp.zeros((rows + 2 * PAD, p.halfp - half), F32)

    for step, k in ORDER:
        {"wz": weights_z, "ys": y_sum, "cv": convs, "xs": x_sum}[step](k)
    conv = acc[0]
    conv = 0.5 * conv
    for h in (0, 1):
        pf_s[h] = conv[pairs * h:pairs * (h + 1)]
    c_pf = send(pf_s.at[other], pf_r, s_loc.at[6], r_loc.at[6], partner)

    def shift(k, d):
        return cks[k, PAD + d:PAD + d + rows, :]

    grad_even = 0.5 * (shift(0, 1) + shift(1, 0) + shift(2, 0) + shift(3, -1) + shift(4, -1))
    grad_odd = 0.5 * (shift(0, 1) + shift(1, 1) + shift(2, 0) + shift(3, 0) + shift(4, -1))
    gain_part = jnp.zeros((1, p.halfp), F32)
    for start, grad in ((0, grad_even), (1, grad_odd)):
        a = strided(af, PAD + start)
        v = a * gain_half
        t = jnp.tanh(ROOT * (v + CUBE * v * v * v))
        slope = 0.5 * (1.0 + t) + 0.5 * v * (1.0 - t * t) * (ROOT * (1.0 + 3.0 * CUBE * v * v))
        pre = grad * slope
        gain_part = gain_part + jnp.sum(pre * a, axis=0, keepdims=True)
        out = pre * gain_half
        for tt in range(p.halfp // 128):
            io[tt, pl.ds(start, rows, 2), :] = out[:, 128 * tt:128 * tt + 128]
    for h in (0, 1):
        gi_s[h] = jnp.concatenate(
            [io[tt, rows * h:rows * (h + 1), :] for tt in range(p.halfp // 128)], axis=1
        ).astype(BF16)
    c_gi = send(gi_s.at[other], gi_r, s_loc.at[7], r_loc.at[7], partner)

    gt[...] = jnp.zeros_like(gt)
    for t in range(tiles):
        gt[0, t:t + 1, :] = gain_part[:, 128 * t:128 * t + 128]
    bias_part = jnp.sum(ct[pl.ds(pl.multiple_of(PAD + pairs * core, 8), pairs), :], axis=0, keepdims=True)
    for t in range(ny):
        gt[0, 4 + t:5 + t, :] = bias_part[:, 128 * t:128 * t + 128]
    c_gx = []
    for flip in (0, 1):
        for dy in range(ny):
            for dx in range(nx):
                i = (flip * ny + dy) * nx + dx
                if i > 0:
                    cc = core if flip == 0 else other
                    c_gx.append(send(gt.at[0], gx.at[i], s_gx.at[i], r_gx.at[i], device(z, at_x(dx), cc, at_y(dy))))

    for g in LATE:
        x_sum(g)

    for c in c_gx:
        c.wait_recv()
    same = gt[0]
    for i in range(1, ny * nx):
        same = same + gx[i]
    flipped = gx[ny * nx]
    for i in range(1, ny * nx):
        flipped = flipped + gx[ny * nx + i]
    first = jnp.where(core == 0, same, flipped)
    second = jnp.where(core == 0, flipped, same)
    gs[0:2, :] = first[0:2]
    gs[2:4, :] = second[0:2]
    gs[4:8, :] = (first + second)[4:8]
    c_gz = []
    for d in range(1, nz):
        c_gz.append(send(gs, gz.at[d - 1], s_gz.at[d - 1], r_gz.at[d - 1], device(at_z(d), x, core, y)))

    c_pf.wait_recv()
    pooled[0] = (pf_s[core] + pf_r[...] + bias[...]).astype(BF16)
    c_gi.wait_recv()
    grad_input[0] = (dot(gi_s[core], mine, NT) + dot(gi_r[...], sel[other], NT)).astype(BF16)

    for c in c_z:
        c.wait_recv()
    for g, (base, length, members) in enumerate(GROUPS):
        final = zo[z_lo, base:base + length, :]
        for d in range(nz - 1):
            final = final + z_r[g][d].astype(F32)
        ya[y, base:base + length, :] = final * factor
    c_ya = []
    for d in range(1, ny):
        c_ya.append(send(ya.at[y], ya.at[y], s_ya.at[d - 1], r_ya.at[d - 1], device(z, x, core, at_y(d))))

    for c in c_gz:
        c.wait_recv()
    total = gs[...]
    for d in range(nz - 1):
        total = total + gz[d]
    total = total * factor
    halves = [
        jnp.concatenate([total[2 * h + t:2 * h + t + 1] for t in range(tiles)], axis=1) for h in (0, 1)
    ]
    grad_gain[...] = picked(halves[0], sel[0], NT) + picked(halves[1], sel[1], NT)
    grad_bias[...] = jnp.concatenate([total[4 + t:5 + t] for t in range(ny)], axis=1)[:, 0:p.cout]

    for c in c_ya:
        c.wait_recv()
    for base, length, members in GROUPS:
        for n, k in enumerate(members):
            row = base + own * n
            wide = jnp.concatenate([ya[t, row:row + own, :] for t in range(ny)], axis=1)
            grad_weight[k] = wide[:, 0:p.cout]
    for c in started:
        c.wait_send()


def build(mesh, plan, factor):
    p = plan
    nx, ny, nz, nzl = p.nx, p.ny, p.nz, p.nzl
    pairs = p.rows // 2
    zrows = sum(length for _, length, _ in GROUPS)
    dma = pltpu.SemaphoreType.DMA
    sems = (
        8, p.taps * len(p.offsets), p.taps * (nx - 1), p.taps * (ny - 1), p.taps * (nx - 1),
        len(GROUPS) * (nz - 1), ny - 1, 2 * nx * ny, nz - 1,
    )
    scratch = [
        pltpu.VMEM((p.rows, p.cin), BF16),
        pltpu.VMEM((pairs, p.cout), BF16),
        pltpu.VMEM((2, 16, p.cin), BF16),
        pltpu.VMEM((2, 16, p.cout), BF16),
        pltpu.VMEM((2, p.cin, p.halfp), BF16),
        pltpu.VMEM((p.halfp // 128, 2 * p.rows + 2 * PAD, 128), F32),
        pltpu.VMEM((p.halfp // 128, 2 * p.rows + 2 * PAD, 128), F32),
        pltpu.VMEM((p.rows + 2 * PAD, p.coutp), F32),
        pltpu.VMEM((nzl, p.taps, p.own, p.cout), BF16),
        pltpu.VMEM((2, p.block, p.cout), F32),
        pltpu.VMEM((nx, p.taps, p.block, p.cout), BF16),
        pltpu.VMEM((ny, p.taps, p.half, 128), BF16),
        pltpu.VMEM((ny, p.taps, p.half, 128), F32),
        pltpu.VMEM((ny - 1, p.taps, p.half, 128), BF16),
        pltpu.VMEM((nx, p.taps, p.block, 128), BF16),
        pltpu.VMEM((nx, p.taps, p.block, 128), F32),
        pltpu.VMEM((nx - 1, p.taps, p.block, 128), BF16),
        pltpu.VMEM((nzl, zrows, 128), F32),
        *[pltpu.VMEM((nzl, length, 128), BF16) for _, length, _ in GROUPS],
        *[pltpu.VMEM((nz - 1, length, 128), BF16) for _, length, _ in GROUPS],
        pltpu.VMEM((ny, zrows, 128), F32),
        pltpu.VMEM((p.taps, p.rows + 2 * PAD, p.halfp), F32),
        pltpu.VMEM((p.halfp // 128, 2 * p.rows, 128), F32),
        pltpu.VMEM((2, p.rows, p.halfp), BF16),
        pltpu.VMEM((p.rows, p.halfp), BF16),
        pltpu.VMEM((2, pairs, p.cout), F32),
        pltpu.VMEM((pairs, p.cout), F32),
        pltpu.VMEM((2 * nx * ny, 8, 128), F32),
        pltpu.VMEM((1, 8, 128), F32),
        pltpu.VMEM((8, 128), F32),
        pltpu.VMEM((nz - 1, 8, 128), F32),
    ]
    for n in sems:
        scratch += [dma((n,)), dma((n,))]
    vmem = pl.BlockSpec(memory_space=pltpu.VMEM)

    def per_device(activ, gain, weight, bias, cotangent):
        outs = pl.pallas_call(
            functools.partial(kernel, p, factor),
            out_shape=(
                jax.ShapeDtypeStruct((1, pairs, p.cout), BF16),
                jax.ShapeDtypeStruct((1, p.rows, p.cin), BF16),
                jax.ShapeDtypeStruct((p.taps, p.own, p.cout), F32),
                jax.ShapeDtypeStruct((1, p.cin), F32),
                jax.ShapeDtypeStruct((1, p.cout), F32),
            ),
            in_specs=[vmem] * 5,
            out_specs=(vmem,) * 5,
            scratch_shapes=scratch,
            compiler_params=pltpu.CompilerParams(collective_id=0, has_side_effects=True),
        )(activ, gain.reshape(1, -1), weight, bias.reshape(1, -1), cotangent)
        return (*outs[:3], outs[3].reshape(-1), outs[4].reshape(-1))

    in_specs = (P("batch", "seq", None), P(), P(None, "seq", None), P(), P("batch", "seq", None))
    out_specs = (P("batch", "seq", None), P("batch", "seq", None), P(None, "seq", None), P(), P())
    return jax.shard_map(per_device, mesh=mesh, in_specs=in_specs, out_specs=out_specs, check_vma=False)


def solution(mesh):
    return build(mesh, Plan(), float(8 * 8192) ** -0.5)
```

```python
import dataclasses
import functools

import jax
import jax.numpy as jnp
from jax import lax
from jax.experimental import pallas as pl
from jax.experimental.pallas import tpu as pltpu
from jax.sharding import PartitionSpec as P

MESH = pl.DeviceIdType.MESH
F32 = jnp.float32
BF16 = jnp.bfloat16
ROOT = 0.7978845608028654
CUBE = 0.044715
PAD = 8


@dataclasses.dataclass(frozen=True)
class Plan:
    nx: int = 4
    ny: int = 4
    nzl: int = 8
    nzh: int = 2
    own: int = 6
    taps: int = 5
    rows: int = 128
    cout: int = 448

    @property
    def nz(self):
        return self.nzl * self.nzh

    @property
    def cin(self):
        return self.own * self.nzl * self.nx * 2

    @property
    def block(self):
        return self.own * self.nzl

    @property
    def half(self):
        return self.block * self.nx

    @property
    def halfp(self):
        return -(-self.half // 128) * 128

    @property
    def coutp(self):
        return self.ny * 128

    @property
    def offsets(self):
        far = self.nzl // 2
        return tuple(range(1, far + 1)) + tuple(-o for o in range(1, self.nzl - far))


def dot(a, b, dims):
    return lax.dot_general(a, b, (dims, ((), ())), preferred_element_type=F32)


def picked(row, ones, dims):
    first = row.astype(BF16)
    rest = row - first.astype(F32)
    second = rest.astype(BF16)
    third = (rest - second.astype(F32)).astype(BF16)
    pieces = [jnp.broadcast_to(v.astype(F32), (8, row.shape[1])) for v in (first, second, third)]
    line = lax.broadcasted_iota(jnp.int32, pieces[0].shape, 0)
    rows = jnp.where(line == 0, pieces[0], jnp.where(line == 1, pieces[1], jnp.where(line == 2, pieces[2], 0.0)))
    out = dot(rows.astype(BF16), ones, dims)
    return out[0:1] + out[1:2] + out[2:3]


NN = ((1,), (0,))
NT = ((1,), (1,))
TN = ((0,), (0,))


TAPS = (2, 1, 3, 0, 4)
GROUPS = ((0, 24, (2, 1, 3, 0)), (24, 8, (4,)))
VIA_Z = (3, 4)
ORDER = (
    ("xf", 0), ("xf", 1), ("wz", 0), ("wz", 1), ("wz", 2), ("ys", 0), ("ys", 1), ("cv", 0), ("ys", 2), ("cv", 1),
    ("ys", 3), ("cv", 2), ("ys", 4), ("zf", 0), ("cv", 3), ("zf", 1), ("cv", 4),
)
LATE = (0, 1)


def kernel(
    plan, factor,
    activ_h, gain_h, weight_h, bias_h, cot_h_,
    pooled, grad_input, grad_weight, grad_gain, grad_bias,
    activ, gain, weight, bias, cot, s_in, act_p, cot_p, act_h, cot_h, sel, af, gf, ct, zb, wf, wx, dws, dwo, yr, xs, xo, xr, zo, zs0, zs1, zr0, zr1, ya, xb, xp, zx, wg, wh,
    cks, io, gi_s, gi_r, pf_s, pf_r, gx, gt, gs, gz,
    s_loc, r_loc, s_az, r_az, s_ax, r_ax, s_y, r_y, s_x, r_x, s_z, r_z, s_ya, r_ya, s_gx, r_gx, s_gz, r_gz, s_xf, r_xf, s_zf, r_zf,
):
    p = plan
    nx, ny, nz, nzl = p.nx, p.ny, p.nz, p.nzl
    rows, half, block, own, taps = p.rows, p.half, p.block, p.own, p.taps
    pairs = rows // 2
    seq, batch = lax.axis_index("seq"), lax.axis_index("batch")
    core = seq % 2
    x = (seq // 2) % nx
    z_lo = seq // (2 * nx)
    z_hi = batch % p.nzh
    y = batch // p.nzh
    z = z_hi * nzl + z_lo
    sign = 1 - 2 * core
    other = 1 - core

    def device(zz, xx, cc, yy):
        return ((zz % nzl) * (2 * nx) + xx * 2 + cc, yy * p.nzh + zz // nzl)

    def at_z(d):
        return (z + d + nz) % nz

    def at_x(d):
        return (x + d) % nx

    def at_y(d):
        return (y + d) % ny

    chip = z * nx + x
    chips = nz * nx
    nxt = (chip + 1) % chips
    prv = (chip + chips - 1) % chips

    partner = device(z, x, other, y)

    def chip_core(c, cc):
        return device(c // nx, c % nx, cc, y)

    barrier = pltpu.get_barrier_semaphore()
    peers = [partner]
    peers += [device(z, at_x(d), cc, y) for d in range(1, nx) for cc in (core, other)]
    peers += [device(z, x, core, at_y(d)) for d in range(1, ny)]
    far = nzl // 2
    peers += [device(at_z(s * o), x, core, y) for o in range(1, far + 1) for s in (1, -1)]
    peers += [chip_core(c, cc) for c in (nxt, prv) for cc in (0, 1)]
    for peer in peers:
        pl.semaphore_signal(barrier, inc=1, device_id=peer, device_id_type=MESH)

    loads = [
        pltpu.make_async_copy(src, dst, s_in.at[i])
        for i, (src, dst) in enumerate(
            ((activ_h.at[0], activ.at[0]), (gain_h, gain), (weight_h, weight), (bias_h, bias), (cot_h_.at[0], cot.at[0]))
        )
    ]
    for load in loads:
        load.start()
    q = lax.broadcasted_iota(jnp.int32, (8, p.halfp), 1)
    chan = own * ((q % block) // own * (2 * nx) + (q // block) * 2) + q % own
    chan = jnp.where(q < half, chan, 2 * p.cin)[0:1]
    r = lax.broadcasted_iota(jnp.int32, (p.cin, p.halfp), 0)
    sel[0] = jnp.where(r == chan, 1.0, 0.0).astype(BF16)
    sel[1] = jnp.where(r == chan + own, 1.0, 0.0).astype(BF16)
    mine = sel[core]

    ct[...] = jnp.zeros_like(ct)
    for load in loads:
        load.wait()
    tiles = p.halfp // 128

    def put(start, value):
        for t in range(tiles):
            af[t, pl.ds(start, value.shape[0]), :] = value[:, 128 * t:128 * t + 128]

    put(pl.multiple_of(PAD + rows * core, 8), dot(activ[0], mine, NN))
    ct[pl.ds(pl.multiple_of(PAD + pairs * core, 8), pairs), 0:p.cout] = cot[0].astype(F32)
    gain_half = picked(gain[...].reshape(1, p.cin), mine, NN)

    pl.semaphore_wait(barrier, len(peers))

    started = []

    def send(src, dst, s, r_, to):
        copy = pltpu.make_async_remote_copy(
            src_ref=src, dst_ref=dst, send_sem=s, recv_sem=r_, device_id=to, device_id_type=MESH
        )
        copy.start()
        started.append(copy)
        return copy

    c_act = send(activ.at[0], act_p, s_loc.at[0], r_loc.at[0], partner)
    c_cot = send(cot.at[0], cot_p, s_loc.at[1], r_loc.at[1], partner)
    edge = 16
    up_chip = jnp.where(core == 1, nxt, prv)
    side = core
    halos = []
    a_edge = pl.ds(pl.multiple_of(core * (rows - edge), edge), edge)
    c_edge = pl.ds(pl.multiple_of(core * (pairs - edge), edge), edge)
    for i, cc in enumerate((0, 1)):
        to = chip_core(up_chip, cc)
        halos.append(send(activ.at[0, a_edge], act_h.at[side], s_loc.at[2 + i], r_loc.at[2 + side], to))
        halos.append(send(cot.at[0, c_edge], cot_h.at[side], s_loc.at[4 + i], r_loc.at[4 + side], to))
    n_off = len(p.offsets)
    c_az = []
    c_xf = []
    for n, k in enumerate(VIA_Z):
        for d in range(1, nx):
            j = (nx - 1) * n + d - 1
            c_xf.append(send(weight.at[k], xb.at[n, x], s_xf.at[j], r_xf.at[j], device(z, at_x(d), core, y)))
        xb[n, x] = weight[k]
    for k in range(taps - len(VIA_Z)):
        for i, o in enumerate(p.offsets):
            j = k * n_off + i
            c_az.append(send(weight.at[k], zb.at[z_lo, k], s_az.at[j], r_az.at[j], device(at_z(sign * o), x, core, y)))
    zb[z_lo] = weight[...]

    def activate(start, count):
        for t in range(tiles):
            v = af[t, start:start + count, :] * gain_half[:, 128 * t:128 * t + 128]
            gf[t, start:start + count, :] = (
                0.5 * v * (1.0 + jnp.tanh(ROOT * (v + CUBE * v * v * v)))
            ).astype(BF16).astype(F32)

    def strided(ref, start):
        return jnp.concatenate([ref[t, pl.ds(start, rows, 2), :] for t in range(tiles)], axis=1)

    def cot_shift(d):
        return ct[PAD + d:PAD + d + rows, :].astype(BF16)

    c_y = [None] * taps

    def y_send(k, part):
        for t in range(ny):
            dwo[t, k] = part[:, 128 * t:128 * t + 128]
            dws[t, k] = part[:, 128 * t:128 * t + 128].astype(BF16)
        c_y[k] = []
        for d in range(1, ny):
            i = (ny - 1) * k + d - 1
            c_y[k].append(send(dws.at[at_y(d), k], yr.at[d - 1, k], s_y.at[i], r_y.at[i], device(z, x, core, at_y(d))))

    c_act.wait_recv()
    put(pl.multiple_of(PAD + rows * other, 8), dot(act_p[...], mine, NN))
    c_cot.wait_recv()
    ct[pl.ds(pl.multiple_of(PAD + pairs * other, 8), pairs), 0:p.cout] = cot_p[...].astype(F32)
    activate(PAD, 2 * rows)
    even, odd = strided(gf, PAD).astype(BF16), strided(gf, PAD + 1).astype(BF16)
    here = cot_shift(0)
    e0, o0 = dot(even, here, TN)[0:half], dot(odd, here, TN)[0:half]
    y_send(2, 0.5 * (e0 + o0))

    for s in (0, 1):
        for src, dst, i in ((activ.at[0, a_edge], act_h, 2), (cot.at[0, c_edge], cot_h, 4)):
            pltpu.make_async_remote_copy(
                src_ref=src, dst_ref=dst.at[s], send_sem=s_loc.at[i], recv_sem=r_loc.at[i + s],
                device_id=partner, device_id_type=MESH,
            ).wait_recv()
    place = z_lo * nx + x
    before = jnp.where(place > 0, 1.0, 0.0).astype(F32)
    after = jnp.where(place < nzl * nx - 1, 1.0, 0.0).astype(F32)
    ct[0:PAD, 0:p.cout] = (cot_h[1].astype(F32) * before)[edge - PAD:edge]
    ct[PAD + rows:, 0:p.cout] = (cot_h[0].astype(F32) * after)[0:PAD]
    up, down = cot_shift(1), cot_shift(-1)
    o_up = dot(odd, up, TN)[0:half]
    y_send(1, 0.5 * (e0 + o_up))
    e_down = dot(even, down, TN)[0:half]
    y_send(3, 0.5 * (e_down + o0))
    y_send(0, 0.5 * (dot(even, up, TN)[0:half] + o_up))
    y_send(4, 0.5 * (e_down + dot(odd, down, TN)[0:half]))
    put(0, (dot(act_h[1], mine, NN) * before)[edge - PAD:edge])
    put(PAD + 2 * rows, (dot(act_h[0], mine, NN) * after)[0:PAD])
    activate(0, PAD)
    activate(PAD + 2 * rows, PAD)

    c_ax = []

    def weights_z(k):
        for c in c_az[n_off * k:n_off * (k + 1)]:
            c.wait_recv()
        for zz in range(nzl):
            wf[k % 2, own * zz:own * (zz + 1)] = zb[zz, k].astype(F32)
        wx[x, k] = wf[k % 2].astype(BF16)
        for d in range(1, nx):
            i = (nx - 1) * k + d - 1
            c_ax.append(send(wx.at[x, k], wx.at[x, k], s_ax.at[i], r_ax.at[i], device(z, at_x(d), core, y)))

    c_zf = []

    def weights_x(n):
        for c in c_xf[(nx - 1) * n:(nx - 1) * (n + 1)]:
            c.wait_recv()
        for xx in range(nx):
            wg[n, own * xx:own * (xx + 1)] = xb[n, xx].astype(F32)
        xp[n] = wg[n].astype(BF16)
        for i, o in enumerate(p.offsets):
            j = n * n_off + i
            c_zf.append(send(xp.at[n], zx.at[n, z_lo], s_zf.at[j], r_zf.at[j], device(at_z(sign * o), x, core, y)))
        zx[n, z_lo] = xp[n]

    def weights_last(n):
        for c in c_zf[n_off * n:n_off * (n + 1)]:
            c.wait_recv()
        for zz in range(nzl):
            rows_z = zx[n, zz].astype(F32)
            for xx in range(nx):
                wh[xx, own * zz:own * (zz + 1)] = rows_z[own * xx:own * (xx + 1)]
        for xx in range(nx):
            wx[xx, VIA_Z[n]] = wh[xx].astype(BF16)

    c_x = {}

    def y_sum(n):
        k = TAPS[n]
        for c in c_y[k]:
            c.wait_recv()
        total = dwo[y, k]
        for d in range(ny - 1):
            total = total + yr[d, k].astype(F32)
        for xx in range(nx):
            piece = total[block * xx:block * (xx + 1)]
            xo[xx, k] = piece
            xs[xx, k] = piece.astype(BF16)
        c_x[k] = []
        for d in range(1, nx):
            i = (nx - 1) * k + d - 1
            c_x[k].append(send(xs.at[at_x(d), k], xr.at[d - 1, k], s_x.at[i], r_x.at[i], device(z, at_x(d), core, y)))

    z_s, z_r = (zs0, zs1), (zr0, zr1)
    c_z = []

    def x_sum(g):
        base, length, members = GROUPS[g]
        zo[:, base:base + length, :] = jnp.zeros((nzl, length, 128), F32)
        for n, k in enumerate(members):
            for c in c_x[k]:
                c.wait_recv()
            total = xo[x, k]
            for d in range(nx - 1):
                total = total + xr[d, k].astype(F32)
            for zz in range(nzl):
                zo[zz, base + own * n:base + own * (n + 1), :] = total[own * zz:own * (zz + 1)]
        z_s[g][...] = zo[:, base:base + length, :].astype(BF16)
        for d in range(1, nz):
            i = (nz - 1) * g + d - 1
            c_z.append(
                send(z_s[g].at[at_z(d) % nzl], z_r[g].at[d - 1], s_z.at[i], r_z.at[i], device(at_z(d), x, core, y))
            )

    acc = [None]
    cot_all = ct[:, 0:p.cout].astype(BF16)
    shifted = [strided(gf, PAD - 2 + j)[:, 0:half].astype(BF16) for j in range(taps + 1)]

    def convs(k):
        if k not in VIA_Z:
            for c in c_ax[(nx - 1) * k:(nx - 1) * (k + 1)]:
                c.wait_recv()
        w = wx[:, k].reshape(half, p.cout)
        add = dot(shifted[k], w, NN) + dot(shifted[k + 1], w, NN)
        acc[0] = add if acc[0] is None else acc[0] + add
        cks[k, :, 0:half] = dot(cot_all, w, NT)
        if half < p.halfp:
            cks[k, :, half:] = jnp.zeros((rows + 2 * PAD, p.halfp - half), F32)

    for step, k in ORDER:
        {"wz": weights_z, "ys": y_sum, "cv": convs, "xs": x_sum, "xf": weights_x, "zf": weights_last}[step](k)
    conv = acc[0]
    conv = 0.5 * conv
    for h in (0, 1):
        pf_s[h] = conv[pairs * h:pairs * (h + 1)]
    c_pf = send(pf_s.at[other], pf_r, s_loc.at[6], r_loc.at[6], partner)

    def shift(k, d):
        return cks[k, PAD + d:PAD + d + rows, :]

    grad_even = 0.5 * (shift(0, 1) + shift(1, 0) + shift(2, 0) + shift(3, -1) + shift(4, -1))
    grad_odd = 0.5 * (shift(0, 1) + shift(1, 1) + shift(2, 0) + shift(3, 0) + shift(4, -1))
    gain_part = jnp.zeros((1, p.halfp), F32)
    for start, grad in ((0, grad_even), (1, grad_odd)):
        a = strided(af, PAD + start)
        v = a * gain_half
        t = jnp.tanh(ROOT * (v + CUBE * v * v * v))
        slope = 0.5 * (1.0 + t) + 0.5 * v * (1.0 - t * t) * (ROOT * (1.0 + 3.0 * CUBE * v * v))
        pre = grad * slope
        gain_part = gain_part + jnp.sum(pre * a, axis=0, keepdims=True)
        out = pre * gain_half
        for tt in range(p.halfp // 128):
            io[tt, pl.ds(start, rows, 2), :] = out[:, 128 * tt:128 * tt + 128]
    for h in (0, 1):
        gi_s[h] = jnp.concatenate(
            [io[tt, rows * h:rows * (h + 1), :] for tt in range(p.halfp // 128)], axis=1
        ).astype(BF16)
    c_gi = send(gi_s.at[other], gi_r, s_loc.at[7], r_loc.at[7], partner)

    gt[...] = jnp.zeros_like(gt)
    for t in range(tiles):
        gt[0, t:t + 1, :] = gain_part[:, 128 * t:128 * t + 128]
    bias_part = jnp.sum(ct[pl.ds(pl.multiple_of(PAD + pairs * core, 8), pairs), :], axis=0, keepdims=True)
    for t in range(ny):
        gt[0, 4 + t:5 + t, :] = bias_part[:, 128 * t:128 * t + 128]
    c_gx = []
    for flip in (0, 1):
        for dy in range(ny):
            for dx in range(nx):
                i = (flip * ny + dy) * nx + dx
                if i > 0:
                    cc = core if flip == 0 else other
                    c_gx.append(send(gt.at[0], gx.at[i], s_gx.at[i], r_gx.at[i], device(z, at_x(dx), cc, at_y(dy))))

    for g in LATE:
        x_sum(g)

    for c in c_gx:
        c.wait_recv()
    same = gt[0]
    for i in range(1, ny * nx):
        same = same + gx[i]
    flipped = gx[ny * nx]
    for i in range(1, ny * nx):
        flipped = flipped + gx[ny * nx + i]
    first = jnp.where(core == 0, same, flipped)
    second = jnp.where(core == 0, flipped, same)
    gs[0:2, :] = first[0:2]
    gs[2:4, :] = second[0:2]
    gs[4:8, :] = (first + second)[4:8]
    c_gz = []
    for d in range(1, nz):
        c_gz.append(send(gs, gz.at[d - 1], s_gz.at[d - 1], r_gz.at[d - 1], device(at_z(d), x, core, y)))

    c_pf.wait_recv()
    pooled[0] = (pf_s[core] + pf_r[...] + bias[...].reshape(1, p.cout)).astype(BF16)
    c_gi.wait_recv()
    grad_input[0] = (dot(gi_s[core], mine, NT) + dot(gi_r[...], sel[other], NT)).astype(BF16)

    for c in c_z:
        c.wait_recv()
    for g, (base, length, members) in enumerate(GROUPS):
        final = zo[z_lo, base:base + length, :]
        for d in range(nz - 1):
            final = final + z_r[g][d].astype(F32)
        ya[y, base:base + length, :] = final * factor
    c_ya = []
    for d in range(1, ny):
        c_ya.append(send(ya.at[y], ya.at[y], s_ya.at[d - 1], r_ya.at[d - 1], device(z, x, core, at_y(d))))

    for c in c_gz:
        c.wait_recv()
    total = gs[...]
    for d in range(nz - 1):
        total = total + gz[d]
    total = total * factor
    halves = [
        jnp.concatenate([total[2 * h + t:2 * h + t + 1] for t in range(tiles)], axis=1) for h in (0, 1)
    ]
    grad_gain[...] = (picked(halves[0], sel[0], NT) + picked(halves[1], sel[1], NT)).reshape(p.cin)
    grad_bias[...] = jnp.concatenate([total[4 + t:5 + t] for t in range(ny)], axis=1)[:, 0:p.cout].reshape(p.cout)

    for c in c_ya:
        c.wait_recv()
    for base, length, members in GROUPS:
        for n, k in enumerate(members):
            row = base + own * n
            wide = jnp.concatenate([ya[t, row:row + own, :] for t in range(ny)], axis=1)
            grad_weight[k] = wide[:, 0:p.cout]
    for c in started:
        c.wait_send()


def hand_over(*refs):
    for src, dst in zip(refs[:5], refs[5:]):
        dst[...] = src[...]


def build(mesh, plan, factor):
    p = plan
    nx, ny, nz, nzl = p.nx, p.ny, p.nz, p.nzl
    pairs = p.rows // 2
    zrows = sum(length for _, length, _ in GROUPS)
    dma = pltpu.SemaphoreType.DMA
    sems = (
        8, p.taps * len(p.offsets), p.taps * (nx - 1), p.taps * (ny - 1), p.taps * (nx - 1),
        len(GROUPS) * (nz - 1), ny - 1, 2 * nx * ny, nz - 1,
        len(VIA_Z) * (nx - 1), len(VIA_Z) * len(p.offsets),
    )
    scratch = [
        pltpu.VMEM((1, p.rows, p.cin), BF16),
        pltpu.VMEM((p.cin,), F32),
        pltpu.VMEM((p.taps, p.own, p.cout), BF16),
        pltpu.VMEM((p.cout,), F32),
        pltpu.VMEM((1, pairs, p.cout), BF16),
        dma((5,)),
        pltpu.VMEM((p.rows, p.cin), BF16),
        pltpu.VMEM((pairs, p.cout), BF16),
        pltpu.VMEM((2, 16, p.cin), BF16),
        pltpu.VMEM((2, 16, p.cout), BF16),
        pltpu.VMEM((2, p.cin, p.halfp), BF16),
        pltpu.VMEM((p.halfp // 128, 2 * p.rows + 2 * PAD, 128), F32),
        pltpu.VMEM((p.halfp // 128, 2 * p.rows + 2 * PAD, 128), F32),
        pltpu.VMEM((p.rows + 2 * PAD, p.coutp), F32),
        pltpu.VMEM((nzl, p.taps, p.own, p.cout), BF16),
        pltpu.VMEM((2, p.block, p.cout), F32),
        pltpu.VMEM((nx, p.taps, p.block, p.cout), BF16),
        pltpu.VMEM((ny, p.taps, p.half, 128), BF16),
        pltpu.VMEM((ny, p.taps, p.half, 128), F32),
        pltpu.VMEM((ny - 1, p.taps, p.half, 128), BF16),
        pltpu.VMEM((nx, p.taps, p.block, 128), BF16),
        pltpu.VMEM((nx, p.taps, p.block, 128), F32),
        pltpu.VMEM((nx - 1, p.taps, p.block, 128), BF16),
        pltpu.VMEM((nzl, zrows, 128), F32),
        *[pltpu.VMEM((nzl, length, 128), BF16) for _, length, _ in GROUPS],
        *[pltpu.VMEM((nz - 1, length, 128), BF16) for _, length, _ in GROUPS],
        pltpu.VMEM((ny, zrows, 128), F32),
        pltpu.VMEM((len(VIA_Z), nx, p.own, p.cout), BF16),
        pltpu.VMEM((len(VIA_Z), p.own * nx, p.cout), BF16),
        pltpu.VMEM((len(VIA_Z), nzl, p.own * nx, p.cout), BF16),
        pltpu.VMEM((len(VIA_Z), p.own * nx, p.cout), F32),
        pltpu.VMEM((nx, p.block, p.cout), F32),
        pltpu.VMEM((p.taps, p.rows + 2 * PAD, p.halfp), F32),
        pltpu.VMEM((p.halfp // 128, 2 * p.rows, 128), F32),
        pltpu.VMEM((2, p.rows, p.halfp), BF16),
        pltpu.VMEM((p.rows, p.halfp), BF16),
        pltpu.VMEM((2, pairs, p.cout), F32),
        pltpu.VMEM((pairs, p.cout), F32),
        pltpu.VMEM((2 * nx * ny, 8, 128), F32),
        pltpu.VMEM((1, 8, 128), F32),
        pltpu.VMEM((8, 128), F32),
        pltpu.VMEM((nz - 1, 8, 128), F32),
    ]
    for n in sems:
        scratch += [dma((n,)), dma((n,))]
    vmem = pl.BlockSpec(memory_space=pltpu.VMEM)

    hbm = pl.BlockSpec(memory_space=pl.ANY)
    shapes = (
        jax.ShapeDtypeStruct((1, pairs, p.cout), BF16),
        jax.ShapeDtypeStruct((1, p.rows, p.cin), BF16),
        jax.ShapeDtypeStruct((p.taps, p.own, p.cout), F32),
        jax.ShapeDtypeStruct((p.cin,), F32),
        jax.ShapeDtypeStruct((p.cout,), F32),
    )

    def per_device(activ, gain, weight, bias, cotangent):
        outs = pl.pallas_call(
            functools.partial(kernel, p, factor),
            out_shape=shapes,
            in_specs=[hbm] * 5,
            out_specs=(vmem,) * 5,
            scratch_shapes=scratch,
            compiler_params=pltpu.CompilerParams(collective_id=0, has_side_effects=True),
        )(activ, gain, weight, bias, cotangent)
        return pl.pallas_call(
            hand_over, out_shape=shapes, in_specs=[vmem] * 5, out_specs=(vmem,) * 5
        )(*outs)

    in_specs = (P("batch", "seq", None), P(), P(None, "seq", None), P(), P("batch", "seq", None))
    out_specs = (P("batch", "seq", None), P("batch", "seq", None), P(None, "seq", None), P(), P())
    return jax.shard_map(per_device, mesh=mesh, in_specs=in_specs, out_specs=out_specs, check_vma=False)


def solution(mesh):
    return build(mesh, Plan(), float(8 * 8192) ** -0.5)
```

```python
import dataclasses
import functools

import jax
import jax.numpy as jnp
from jax import lax
from jax.experimental import pallas as pl
from jax.experimental.pallas import tpu as pltpu
from jax.sharding import PartitionSpec as P

MESH = pl.DeviceIdType.MESH
F32 = jnp.float32
BF16 = jnp.bfloat16
ROOT = 0.7978845608028654
CUBE = 0.044715
PAD = 8


@dataclasses.dataclass(frozen=True)
class Plan:
    nx: int = 4
    ny: int = 4
    nzl: int = 8
    nzh: int = 2
    own: int = 6
    taps: int = 5
    rows: int = 128
    cout: int = 448

    @property
    def nz(self):
        return self.nzl * self.nzh

    @property
    def cin(self):
        return self.own * self.nzl * self.nx * 2

    @property
    def block(self):
        return self.own * self.nzl

    @property
    def half(self):
        return self.block * self.nx

    @property
    def halfp(self):
        return -(-self.half // 128) * 128

    @property
    def coutp(self):
        return self.ny * 128

    @property
    def offsets(self):
        far = self.nzl // 2
        return tuple(range(1, far + 1)) + tuple(-o for o in range(1, self.nzl - far))


def dot(a, b, dims):
    return lax.dot_general(a, b, (dims, ((), ())), preferred_element_type=F32)


def picked(row, ones, dims):
    first = row.astype(BF16)
    rest = row - first.astype(F32)
    second = rest.astype(BF16)
    third = (rest - second.astype(F32)).astype(BF16)
    pieces = [jnp.broadcast_to(v.astype(F32), (8, row.shape[1])) for v in (first, second, third)]
    line = lax.broadcasted_iota(jnp.int32, pieces[0].shape, 0)
    rows = jnp.where(line == 0, pieces[0], jnp.where(line == 1, pieces[1], jnp.where(line == 2, pieces[2], 0.0)))
    out = dot(rows.astype(BF16), ones, dims)
    return out[0:1] + out[1:2] + out[2:3]


NN = ((1,), (0,))
NT = ((1,), (1,))
TN = ((0,), (0,))


TAPS = (2, 1, 3, 0)
X_FIRST = 4
GROUPS = ((0, 24, (2, 1, 3, 4)), (24, 8, (0,)))
VIA_Z = (3, 4)
ORDER = (
    ("xf", 0), ("xf", 1), ("wz", 0), ("wz", 1), ("wz", 2), ("ys", 0), ("ys", 1), ("x1", 0), ("cv", 0), ("ys", 2),
    ("cv", 1), ("ys", 3), ("cv", 2), ("zf", 0), ("cv", 3), ("xs", 0), ("zf", 1), ("cv", 4),
)
LATE = (1,)


def kernel(
    plan, factor,
    activ_h, gain_h, weight_h, bias_h, cot_h_,
    pooled, grad_input, grad_weight, grad_gain, grad_bias,
    activ, gain, weight, bias, cot, s_in, far_sem, act_p, cot_p, act_h, cot_h, sel, af, gf, ct, zb, wf, wx, dws, dwo, yr, xs, xo, xr, zo, zs0, zs1, zr0, zr1, ya, xb, xp, zx, wg, wh,
    cks, io, gi_s, gi_r, pf_s, pf_r, gx, gt, gs, gz, bt, bx, bs, bz, fo, fs, fr, go, gb, gr,
    s_loc, r_loc, s_az, r_az, s_ax, r_ax, s_y, r_y, s_x, r_x, s_z, r_z, s_ya, r_ya, s_gx, r_gx, s_gz, r_gz, s_xf, r_xf, s_zf, r_zf, s_bx, r_bx, s_bz, r_bz, s_f, r_f, s_g, r_g,
):
    p = plan
    nx, ny, nz, nzl = p.nx, p.ny, p.nz, p.nzl
    rows, half, block, own, taps = p.rows, p.half, p.block, p.own, p.taps
    pairs = rows // 2
    seq, batch = lax.axis_index("seq"), lax.axis_index("batch")
    core = seq % 2
    x = (seq // 2) % nx
    z_lo = seq // (2 * nx)
    z_hi = batch % p.nzh
    y = batch // p.nzh
    z = z_hi * nzl + z_lo
    sign = 1 - 2 * core
    other = 1 - core

    def device(zz, xx, cc, yy):
        return ((zz % nzl) * (2 * nx) + xx * 2 + cc, yy * p.nzh + zz // nzl)

    def at_z(d):
        return (z + d + nz) % nz

    def at_x(d):
        return (x + d) % nx

    def at_y(d):
        return (y + d) % ny

    chip = z * nx + x
    chips = nz * nx
    nxt = (chip + 1) % chips
    prv = (chip + chips - 1) % chips

    partner = device(z, x, other, y)

    def chip_core(c, cc):
        return device(c // nx, c % nx, cc, y)

    XFAR = sorted(range(1, nx), key=lambda d: -min(d, nx - d))
    YFAR = sorted(range(1, ny), key=lambda d: -min(d, ny - d))
    ZFAR = sorted(range(1, nz), key=lambda d: -min(d, nz - d))
    SQUARE = sorted(
        ((dy, dx) for dy in range(ny) for dx in range(nx)), key=lambda v: -min(v[0], ny - v[0]) - min(v[1], nx - v[1])
    )
    barrier = pltpu.get_barrier_semaphore()
    peers = [partner]
    peers += [device(z, at_x(d), cc, y) for d in range(1, nx) for cc in (core, other)]
    peers += [device(z, x, core, at_y(d)) for d in range(1, ny)]
    far = nzl // 2
    near = min(2, far)
    peers += [device(at_z(s * o), x, core, y) for o in range(1, near + 1) for s in (1, -1)]
    peers += [chip_core(c, cc) for c in (nxt, prv) for cc in (0, 1)]
    for peer in peers:
        pl.semaphore_signal(barrier, inc=1, device_id=peer, device_id_type=MESH)

    loads = [
        pltpu.make_async_copy(src, dst, s_in.at[i])
        for i, (src, dst) in enumerate(
            ((activ_h.at[0], activ.at[0]), (gain_h, gain), (weight_h, weight), (bias_h, bias), (cot_h_.at[0], cot.at[0]))
        )
    ]
    for load in loads:
        load.start()
    q = lax.broadcasted_iota(jnp.int32, (8, p.halfp), 1)
    chan = own * ((q % block) // own * (2 * nx) + (q // block) * 2) + q % own
    chan = jnp.where(q < half, chan, 2 * p.cin)[0:1]
    r = lax.broadcasted_iota(jnp.int32, (p.cin, p.halfp), 0)
    sel[0] = jnp.where(r == chan, 1.0, 0.0).astype(BF16)
    sel[1] = jnp.where(r == chan + own, 1.0, 0.0).astype(BF16)
    mine = sel[core]

    ct[...] = jnp.zeros_like(ct)
    for load in loads:
        load.wait()
    tiles = p.halfp // 128

    def put(start, value):
        for t in range(tiles):
            af[t, pl.ds(start, value.shape[0]), :] = value[:, 128 * t:128 * t + 128]

    put(pl.multiple_of(PAD + rows * core, 8), dot(activ[0], mine, NN))
    ct[pl.ds(pl.multiple_of(PAD + pairs * core, 8), pairs), 0:p.cout] = cot[0].astype(F32)
    gain_half = picked(gain[...].reshape(1, p.cin), mine, NN)

    pl.semaphore_wait(barrier, len(peers))

    for s in (1, -1):
        pl.semaphore_signal(far_sem, inc=1, device_id=device(at_z(s * near), x, core, y), device_id_type=MESH)

    started = []

    def send(src, dst, s, r_, to):
        copy = pltpu.make_async_remote_copy(
            src_ref=src, dst_ref=dst, send_sem=s, recv_sem=r_, device_id=to, device_id_type=MESH
        )
        copy.start()
        started.append(copy)
        return copy

    def share(src, dst, s, r_, to):
        pltpu.make_async_remote_copy(
            src_ref=src, dst_ref=dst, send_sem=s, recv_sem=r_, device_id=to, device_id_type=MESH
        ).start()

    def whole(region, sem):
        return pltpu.make_async_remote_copy(
            src_ref=region, dst_ref=region, send_sem=sem, recv_sem=sem, device_id=partner, device_id_type=MESH
        )

    def arrived(region, sem):
        whole(region, sem).wait_recv()

    c_act = send(activ.at[0], act_p, s_loc.at[0], r_loc.at[0], partner)
    c_cot = send(cot.at[0], cot_p, s_loc.at[1], r_loc.at[1], partner)
    edge = 16
    up_chip = jnp.where(core == 1, nxt, prv)
    side = core
    halos = []
    a_edge = pl.ds(pl.multiple_of(core * (rows - edge), edge), edge)
    c_edge = pl.ds(pl.multiple_of(core * (pairs - edge), edge), edge)
    for i, cc in enumerate((0, 1)):
        to = chip_core(up_chip, cc)
        halos.append(send(activ.at[0, a_edge], act_h.at[side], s_loc.at[2 + i], r_loc.at[2 + side], to))
        halos.append(send(cot.at[0, c_edge], cot_h.at[side], s_loc.at[4 + i], r_loc.at[4 + side], to))
    n_off = len(p.offsets)
    c_az = []
    for n, k in enumerate(VIA_Z):
        for d in XFAR:
            share(weight.at[k], xb.at[n, x], s_xf.at[0], r_xf.at[n], device(z, at_x(d), core, y))
        xb[n, x] = weight[k]
    direct = range(taps - len(VIA_Z))

    def weights_out(wanted):
        for k in direct:
            for o in sorted(p.offsets, key=lambda v: -abs(v)):
                if (abs(o) <= near) == wanted:
                    to = device(at_z(sign * o), x, core, y)
                    share(weight.at[k], zb.at[z_lo, k], s_az.at[0], r_az.at[k], to)

    weights_out(True)
    zb[z_lo] = weight[...]

    def activate(start, count):
        for t in range(tiles):
            v = af[t, start:start + count, :] * gain_half[:, 128 * t:128 * t + 128]
            gf[t, start:start + count, :] = (
                0.5 * v * (1.0 + jnp.tanh(ROOT * (v + CUBE * v * v * v)))
            ).astype(BF16).astype(F32)

    def strided(ref, start):
        return jnp.concatenate([ref[t, pl.ds(start, rows, 2), :] for t in range(tiles)], axis=1)

    def cot_shift(d):
        return ct[PAD + d:PAD + d + rows, :].astype(BF16)

    def y_send(k, part):
        for t in range(ny):
            dwo[t, k] = part[:, 128 * t:128 * t + 128]
            dws[t, k] = part[:, 128 * t:128 * t + 128].astype(BF16)
        for d in YFAR:
            share(dws.at[at_y(d), k], yr.at[k, d - 1], s_y.at[0], r_y.at[k], device(z, x, core, at_y(d)))

    c_act.wait_recv()
    put(pl.multiple_of(PAD + rows * other, 8), dot(act_p[...], mine, NN))
    c_cot.wait_recv()
    ct[pl.ds(pl.multiple_of(PAD + pairs * other, 8), pairs), 0:p.cout] = cot_p[...].astype(F32)
    bias_part = jnp.sum(ct[PAD:PAD + rows, :], axis=0, keepdims=True)
    for t in range(ny):
        bt[t:t + 1, :] = bias_part[:, 128 * t:128 * t + 128]

    def bias_out():
        for dy, dx in SQUARE:
            i = dy * nx + dx - 1
            if i >= 0:
                share(bt, bx.at[i], s_bx.at[0], r_bx.at[0], device(z, at_x(dx), core, at_y(dy)))

    def bias_sum(_):
        arrived(bx, r_bx.at[0])
        total = bt[...]
        for i in range(nx * ny - 1):
            total = total + bx[i]
        bs[...] = total
        for d in ZFAR:
            share(bs, bz.at[d - 1], s_bz.at[0], r_bz.at[0], device(at_z(d), x, core, y))

    activate(PAD, 2 * rows)
    even, odd = strided(gf, PAD).astype(BF16), strided(gf, PAD + 1).astype(BF16)
    here = cot_shift(0)
    e0, o0 = dot(even, here, TN)[0:half], dot(odd, here, TN)[0:half]
    y_send(2, 0.5 * (e0 + o0))
    pl.semaphore_wait(far_sem, 2)
    weights_out(False)

    for s in (0, 1):
        for src, dst, i in ((activ.at[0, a_edge], act_h, 2), (cot.at[0, c_edge], cot_h, 4)):
            pltpu.make_async_remote_copy(
                src_ref=src, dst_ref=dst.at[s], send_sem=s_loc.at[i], recv_sem=r_loc.at[i + s],
                device_id=partner, device_id_type=MESH,
            ).wait_recv()
    place = z_lo * nx + x
    before = jnp.where(place > 0, 1.0, 0.0).astype(F32)
    after = jnp.where(place < nzl * nx - 1, 1.0, 0.0).astype(F32)
    ct[0:PAD, 0:p.cout] = (cot_h[1].astype(F32) * before)[edge - PAD:edge]
    ct[PAD + rows:, 0:p.cout] = (cot_h[0].astype(F32) * after)[0:PAD]
    up, down = cot_shift(1), cot_shift(-1)
    e_down = dot(even, down, TN)[0:half]
    part = 0.5 * (e_down + dot(odd, down, TN)[0:half])
    for xx in range(nx):
        fo[xx] = part[block * xx:block * (xx + 1)]
        fs[xx] = part[block * xx:block * (xx + 1)].astype(BF16)
    for d in XFAR:
        share(fs.at[at_x(d)], fr.at[d - 1], s_f.at[0], r_f.at[0], device(z, at_x(d), core, y))
    o_up = dot(odd, up, TN)[0:half]
    y_send(1, 0.5 * (e0 + o_up))
    y_send(3, 0.5 * (e_down + o0))
    y_send(0, 0.5 * (dot(even, up, TN)[0:half] + o_up))
    put(0, (dot(act_h[1], mine, NN) * before)[edge - PAD:edge])
    put(PAD + 2 * rows, (dot(act_h[0], mine, NN) * after)[0:PAD])
    activate(0, PAD)
    activate(PAD + 2 * rows, PAD)

    def weights_z(k):
        arrived(zb.at[pl.ds(0, n_off), k], r_az.at[k])
        for zz in range(nzl):
            wf[k % 2, own * zz:own * (zz + 1)] = zb[zz, k].astype(F32)
        wx[x, k] = wf[k % 2].astype(BF16)
        for d in XFAR:
            share(wx.at[x, k], wx.at[x, k], s_ax.at[0], r_ax.at[k], device(z, at_x(d), core, y))

    def weights_x(n):
        arrived(xb.at[n, pl.ds(0, nx - 1)], r_xf.at[n])
        for xx in range(nx):
            wg[n, own * xx:own * (xx + 1)] = xb[n, xx].astype(F32)
        xp[n] = wg[n].astype(BF16)
        for o in sorted(p.offsets, key=lambda v: -abs(v)):
            share(xp.at[n], zx.at[n, z_lo], s_zf.at[0], r_zf.at[n], device(at_z(sign * o), x, core, y))
        zx[n, z_lo] = xp[n]

    def weights_last(n):
        arrived(zx.at[n, pl.ds(0, n_off)], r_zf.at[n])
        for zz in range(nzl):
            rows_z = zx[n, zz].astype(F32)
            for xx in range(nx):
                wh[xx, own * zz:own * (zz + 1)] = rows_z[own * xx:own * (xx + 1)]
        for xx in range(nx):
            wx[xx, VIA_Z[n]] = wh[xx].astype(BF16)

    def y_sum(n):
        k = TAPS[n]
        arrived(yr.at[k], r_y.at[k])
        if n == 0:
            bias_out()
        total = dwo[y, k]
        for d in range(ny - 1):
            total = total + yr[k, d].astype(F32)
        for xx in range(nx):
            piece = total[block * xx:block * (xx + 1)]
            xo[xx, k] = piece
            xs[xx, k] = piece.astype(BF16)
        for d in XFAR:
            share(xs.at[at_x(d), k], xr.at[k, d - 1], s_x.at[0], r_x.at[k], device(z, at_x(d), core, y))

    def x_first(_):
        arrived(fr, r_f.at[0])
        total = fo[x]
        for d in range(nx - 1):
            total = total + fr[d].astype(F32)
        for t in range(ny):
            go[t] = total[:, 128 * t:128 * t + 128]
            gb[t] = total[:, 128 * t:128 * t + 128].astype(BF16)
        for d in YFAR:
            share(gb.at[at_y(d)], gr.at[d - 1], s_g.at[0], r_g.at[0], device(z, x, core, at_y(d)))

    z_s, z_r = (zs0, zs1), (zr0, zr1)
    def x_sum(g):
        base, length, members = GROUPS[g]
        zo[:, base:base + length, :] = jnp.zeros((nzl, length, 128), F32)
        for n, k in enumerate(members):
            if k == X_FIRST:
                arrived(gr, r_g.at[0])
            else:
                arrived(xr.at[k], r_x.at[k])
            total = go[y] if k == X_FIRST else xo[x, k]
            for d in range((ny if k == X_FIRST else nx) - 1):
                total = total + (gr[d] if k == X_FIRST else xr[k, d]).astype(F32)
            for zz in range(nzl):
                zo[zz, base + own * n:base + own * (n + 1), :] = total[own * zz:own * (zz + 1)]
        z_s[g][...] = zo[:, base:base + length, :].astype(BF16)
        for d in ZFAR:
            share(z_s[g].at[at_z(d) % nzl], z_r[g].at[d - 1], s_z.at[g], r_z.at[g], device(at_z(d), x, core, y))

    acc = [None]
    cot_all = ct[:, 0:p.cout].astype(BF16)
    shifted = [strided(gf, PAD - 2 + j)[:, 0:half].astype(BF16) for j in range(taps + 1)]

    def convs(k):
        if k not in VIA_Z:
            arrived(wx.at[pl.ds(0, nx - 1), k], r_ax.at[k])
        w = wx[:, k].reshape(half, p.cout)
        add = dot(shifted[k], w, NN) + dot(shifted[k + 1], w, NN)
        acc[0] = add if acc[0] is None else acc[0] + add
        cks[k, :, 0:half] = dot(cot_all, w, NT)
        if half < p.halfp:
            cks[k, :, half:] = jnp.zeros((rows + 2 * PAD, p.halfp - half), F32)

    for step, k in ORDER:
        {"wz": weights_z, "ys": y_sum, "cv": convs, "xs": x_sum, "xf": weights_x, "zf": weights_last, "x1": x_first}[step](k)
    conv = acc[0]
    conv = 0.5 * conv
    for h in (0, 1):
        pf_s[h] = conv[pairs * h:pairs * (h + 1)]
    c_pf = send(pf_s.at[other], pf_r, s_loc.at[6], r_loc.at[6], partner)

    def shift(k, d):
        return cks[k, PAD + d:PAD + d + rows, :]

    grad_even = 0.5 * (shift(0, 1) + shift(1, 0) + shift(2, 0) + shift(3, -1) + shift(4, -1))
    grad_odd = 0.5 * (shift(0, 1) + shift(1, 1) + shift(2, 0) + shift(3, 0) + shift(4, -1))
    gain_part = jnp.zeros((1, p.halfp), F32)
    for start, grad in ((0, grad_even), (1, grad_odd)):
        a = strided(af, PAD + start)
        v = a * gain_half
        t = jnp.tanh(ROOT * (v + CUBE * v * v * v))
        slope = 0.5 * (1.0 + t) + 0.5 * v * (1.0 - t * t) * (ROOT * (1.0 + 3.0 * CUBE * v * v))
        pre = grad * slope
        gain_part = gain_part + jnp.sum(pre * a, axis=0, keepdims=True)
        out = pre * gain_half
        for tt in range(p.halfp // 128):
            io[tt, pl.ds(start, rows, 2), :] = out[:, 128 * tt:128 * tt + 128]
    for h in (0, 1):
        gi_s[h] = jnp.concatenate(
            [io[tt, rows * h:rows * (h + 1), :] for tt in range(p.halfp // 128)], axis=1
        ).astype(BF16)
    c_gi = send(gi_s.at[other], gi_r, s_loc.at[7], r_loc.at[7], partner)

    for t in range(tiles):
        gt[0, t:t + 1, :] = gain_part[:, 128 * t:128 * t + 128]
    for dy, dx in SQUARE:
        for flip in (0, 1):
            i = (flip * ny + dy) * nx + dx
            if i > 0:
                cc = core if flip == 0 else other
                share(gt.at[0], gx.at[i], s_gx.at[0], r_gx.at[0], device(z, at_x(dx), cc, at_y(dy)))

    for g in LATE:
        x_sum(g)
    bias_sum(0)

    others = gx.at[pl.ds(1, 2 * nx * ny - 1)]
    arrived(others, r_gx.at[0])
    same = gt[0]
    for i in range(1, ny * nx):
        same = same + gx[i]
    flipped = gx[ny * nx]
    for i in range(1, ny * nx):
        flipped = flipped + gx[ny * nx + i]
    first = jnp.where(core == 0, same, flipped)
    second = jnp.where(core == 0, flipped, same)
    gs[0:tiles, :] = first
    gs[tiles:2 * tiles, :] = second
    for d in ZFAR:
        share(gs, gz.at[d - 1], s_gz.at[0], r_gz.at[0], device(at_z(d), x, core, y))

    c_pf.wait_recv()
    pooled[0] = (pf_s[core] + pf_r[...] + bias[...].reshape(1, p.cout)).astype(BF16)
    c_gi.wait_recv()
    grad_input[0] = (dot(gi_s[core], mine, NT) + dot(gi_r[...], sel[other], NT)).astype(BF16)

    for g in range(len(GROUPS)):
        arrived(z_r[g], r_z.at[g])
    for g, (base, length, members) in enumerate(GROUPS):
        final = zo[z_lo, base:base + length, :]
        for d in range(nz - 1):
            final = final + z_r[g][d].astype(F32)
        ya[y, base:base + length, :] = final * factor
    c_ya = []
    for d in range(1, ny):
        c_ya.append(send(ya.at[y], ya.at[y], s_ya.at[d - 1], r_ya.at[d - 1], device(z, x, core, at_y(d))))

    arrived(gz, r_gz.at[0])
    total = gs[...]
    for d in range(nz - 1):
        total = total + gz[d]
    total = total * factor
    halves = [
        jnp.concatenate([total[tiles * h + t:tiles * h + t + 1] for t in range(tiles)], axis=1) for h in (0, 1)
    ]
    grad_gain[...] = (picked(halves[0], sel[0], NT) + picked(halves[1], sel[1], NT)).reshape(p.cin)

    arrived(bz, r_bz.at[0])
    total = bs[...]
    for d in range(nz - 1):
        total = total + bz[d]
    total = total * factor
    grad_bias[...] = jnp.concatenate([total[t:t + 1] for t in range(ny)], axis=1)[:, 0:p.cout].reshape(p.cout)

    for c in c_ya:
        c.wait_recv()
    for base, length, members in GROUPS:
        for n, k in enumerate(members):
            row = base + own * n
            wide = jnp.concatenate([ya[t, row:row + own, :] for t in range(ny)], axis=1)
            grad_weight[k] = wide[:, 0:p.cout]
    for c in started:
        c.wait_send()
    n_direct, n_via, n_y = len(direct), len(VIA_Z), len(TAPS)
    for region, sem in (
        (xb.at[:, pl.ds(0, nx - 1)], s_xf), (zb.at[pl.ds(0, n_off), pl.ds(0, n_direct)], s_az), (yr, s_y), (bx, s_bx),
        (bz, s_bz), (fr, s_f), (gr, s_g), (wx.at[pl.ds(0, nx - 1), pl.ds(0, n_direct)], s_ax),
        (zx.at[:, pl.ds(0, n_off)], s_zf), (xr, s_x), (others, s_gx), (gz, s_gz),
    ):
        whole(region, sem.at[0]).wait_send()
    for g in range(len(GROUPS)):
        whole(z_r[g], s_z.at[g]).wait_send()


def hand_over(*refs):
    for src, dst in zip(refs[:5], refs[5:]):
        dst[...] = src[...]


def build(mesh, plan, factor):
    p = plan
    nx, ny, nz, nzl = p.nx, p.ny, p.nz, p.nzl
    pairs = p.rows // 2
    zrows = sum(length for _, length, _ in GROUPS)
    dma = pltpu.SemaphoreType.DMA
    n_direct, n_via, n_y = p.taps - len(VIA_Z), len(VIA_Z), len(TAPS)
    sems = (
        (8, 8), (1, n_direct), (1, n_direct), (1, n_y), (1, n_y), (len(GROUPS),) * 2, (ny - 1, ny - 1),
        (1, 1), (1, 1), (1, n_via), (1, n_via), (1, 1), (1, 1), (1, 1), (1, 1),
    )
    scratch = [
        pltpu.VMEM((1, p.rows, p.cin), BF16),
        pltpu.VMEM((p.cin,), F32),
        pltpu.VMEM((p.taps, p.own, p.cout), BF16),
        pltpu.VMEM((p.cout,), F32),
        pltpu.VMEM((1, pairs, p.cout), BF16),
        dma((5,)),
        pltpu.SemaphoreType.REGULAR,
        pltpu.VMEM((p.rows, p.cin), BF16),
        pltpu.VMEM((pairs, p.cout), BF16),
        pltpu.VMEM((2, 16, p.cin), BF16),
        pltpu.VMEM((2, 16, p.cout), BF16),
        pltpu.VMEM((2, p.cin, p.halfp), BF16),
        pltpu.VMEM((p.halfp // 128, 2 * p.rows + 2 * PAD, 128), F32),
        pltpu.VMEM((p.halfp // 128, 2 * p.rows + 2 * PAD, 128), F32),
        pltpu.VMEM((p.rows + 2 * PAD, p.coutp), F32),
        pltpu.VMEM((nzl, p.taps, p.own, p.cout), BF16),
        pltpu.VMEM((2, p.block, p.cout), F32),
        pltpu.VMEM((nx, p.taps, p.block, p.cout), BF16),
        pltpu.VMEM((ny, p.taps, p.half, 128), BF16),
        pltpu.VMEM((ny, p.taps, p.half, 128), F32),
        pltpu.VMEM((len(TAPS), ny - 1, p.half, 128), BF16),
        pltpu.VMEM((nx, p.taps, p.block, 128), BF16),
        pltpu.VMEM((nx, p.taps, p.block, 128), F32),
        pltpu.VMEM((len(TAPS), nx - 1, p.block, 128), BF16),
        pltpu.VMEM((nzl, zrows, 128), F32),
        *[pltpu.VMEM((nzl, length, 128), BF16) for _, length, _ in GROUPS],
        *[pltpu.VMEM((nz - 1, length, 128), BF16) for _, length, _ in GROUPS],
        pltpu.VMEM((ny, zrows, 128), F32),
        pltpu.VMEM((len(VIA_Z), nx, p.own, p.cout), BF16),
        pltpu.VMEM((len(VIA_Z), p.own * nx, p.cout), BF16),
        pltpu.VMEM((len(VIA_Z), nzl, p.own * nx, p.cout), BF16),
        pltpu.VMEM((len(VIA_Z), p.own * nx, p.cout), F32),
        pltpu.VMEM((nx, p.block, p.cout), F32),
        pltpu.VMEM((p.taps, p.rows + 2 * PAD, p.halfp), F32),
        pltpu.VMEM((p.halfp // 128, 2 * p.rows, 128), F32),
        pltpu.VMEM((2, p.rows, p.halfp), BF16),
        pltpu.VMEM((p.rows, p.halfp), BF16),
        pltpu.VMEM((2, pairs, p.cout), F32),
        pltpu.VMEM((pairs, p.cout), F32),
        pltpu.VMEM((2 * nx * ny, p.halfp // 128, 128), F32),
        pltpu.VMEM((1, p.halfp // 128, 128), F32),
        pltpu.VMEM((p.halfp // 64, 128), F32),
        pltpu.VMEM((nz - 1, p.halfp // 64, 128), F32),
        pltpu.VMEM((ny, 128), F32),
        pltpu.VMEM((nx * ny - 1, ny, 128), F32),
        pltpu.VMEM((ny, 128), F32),
        pltpu.VMEM((nz - 1, ny, 128), F32),
        pltpu.VMEM((nx, p.block, p.coutp), F32),
        pltpu.VMEM((nx, p.block, p.coutp), BF16),
        pltpu.VMEM((nx - 1, p.block, p.coutp), BF16),
        pltpu.VMEM((ny, p.block, 128), F32),
        pltpu.VMEM((ny, p.block, 128), BF16),
        pltpu.VMEM((ny - 1, p.block, 128), BF16),
    ]
    for sent, received in sems:
        scratch += [dma((sent,)), dma((received,))]
    vmem = pl.BlockSpec(memory_space=pltpu.VMEM)

    hbm = pl.BlockSpec(memory_space=pltpu.HBM)
    shapes = (
        jax.ShapeDtypeStruct((1, pairs, p.cout), BF16),
        jax.ShapeDtypeStruct((1, p.rows, p.cin), BF16),
        jax.ShapeDtypeStruct((p.taps, p.own, p.cout), F32),
        jax.ShapeDtypeStruct((p.cin,), F32),
        jax.ShapeDtypeStruct((p.cout,), F32),
    )

    def per_device(activ, gain, weight, bias, cotangent):
        outs = pl.pallas_call(
            functools.partial(kernel, p, factor),
            out_shape=shapes,
            in_specs=[hbm] * 5,
            out_specs=(vmem,) * 5,
            scratch_shapes=scratch,
            compiler_params=pltpu.CompilerParams(collective_id=0, has_side_effects=True),
        )(activ, gain, weight, bias, cotangent)
        return pl.pallas_call(
            hand_over, out_shape=shapes, in_specs=[vmem] * 5, out_specs=(vmem,) * 5,
        )(*outs)

    in_specs = (P("batch", "seq", None), P(), P(None, "seq", None), P(), P("batch", "seq", None))
    out_specs = (P("batch", "seq", None), P("batch", "seq", None), P(None, "seq", None), P(), P())
    return jax.shard_map(per_device, mesh=mesh, in_specs=in_specs, out_specs=out_specs, check_vma=False)


def solution(mesh):
    return build(mesh, Plan(), float(8 * 8192) ** -0.5)
```

```python
import dataclasses
import functools

import jax
import jax.numpy as jnp
from jax import lax
from jax.experimental import pallas as pl
from jax.experimental.pallas import tpu as pltpu
from jax.sharding import PartitionSpec as P

MESH = pl.DeviceIdType.MESH
F32 = jnp.float32
BF16 = jnp.bfloat16
ROOT = 0.7978845608028654
CUBE = 0.044715
PAD = 8


@dataclasses.dataclass(frozen=True)
class Plan:
    nx: int = 4
    ny: int = 4
    nzl: int = 8
    nzh: int = 2
    own: int = 6
    taps: int = 5
    rows: int = 128
    cout: int = 448

    @property
    def nz(self):
        return self.nzl * self.nzh

    @property
    def cin(self):
        return self.own * self.nzl * self.nx * 2

    @property
    def block(self):
        return self.own * self.nzl

    @property
    def half(self):
        return self.block * self.nx

    @property
    def halfp(self):
        return -(-self.half // 128) * 128

    @property
    def coutp(self):
        return self.ny * 128

    @property
    def offsets(self):
        far = self.nzl // 2
        return tuple(range(1, far + 1)) + tuple(-o for o in range(1, self.nzl - far))


def dot(a, b, dims):
    return lax.dot_general(a, b, (dims, ((), ())), preferred_element_type=F32)


def picked(row, ones, dims):
    first = row.astype(BF16)
    rest = row - first.astype(F32)
    second = rest.astype(BF16)
    third = (rest - second.astype(F32)).astype(BF16)
    pieces = [jnp.broadcast_to(v.astype(F32), (8, row.shape[1])) for v in (first, second, third)]
    line = lax.broadcasted_iota(jnp.int32, pieces[0].shape, 0)
    rows = jnp.where(line == 0, pieces[0], jnp.where(line == 1, pieces[1], jnp.where(line == 2, pieces[2], 0.0)))
    out = dot(rows.astype(BF16), ones, dims)
    return out[0:1] + out[1:2] + out[2:3]


NN = ((1,), (0,))
NT = ((1,), (1,))
TN = ((0,), (0,))


TAPS = (2, 1, 3, 0)
X_FIRST = 4
GROUPS = ((0, 24, (2, 1, 3, 4)), (24, 8, (0,)))
VIA_Z = (3, 4)
ORDER = (
    ("xf", 0), ("xf", 1), ("bx", 0), ("wz", 0), ("wz", 1), ("wz", 2), ("bs", 0), ("ys", 0), ("ys", 1), ("x1", 0), ("cv", 0), ("ys", 2),
    ("cv", 1), ("ys", 3), ("cv", 2), ("zf", 0), ("cv", 3), ("xs", 0), ("zf", 1), ("cv", 4),
)
LATE = (1,)


def kernel(
    plan, factor,
    activ_h, gain_h, weight_h, bias_h, cot_h_,
    pooled, grad_input, grad_weight, grad_gain, grad_bias,
    activ, gain, weight, bias, cot, s_in, far_sem, act_p, cot_p, act_h, cot_h, sel, af, gf, ct, zb, wf, wx, dws, dwo, yr, xs, xo, xr, zo, zs0, zs1, zr0, zr1, ya, xb, xp, zx, wg, wh,
    cks, io, gi_s, gi_r, pf_s, pf_r, gx, gt, gs, gz, bt, bu, bx, bs, bz, fo, fs, fr, go, gb, gr,
    s_loc, r_loc, s_az, r_az, s_ax, r_ax, s_y, r_y, s_x, r_x, s_z, r_z, s_ya, r_ya, s_gx, r_gx, s_gz, r_gz, s_xf, r_xf, s_zf, r_zf, s_bx, r_bx, s_bz, r_bz, s_f, r_f, s_g, r_g,
):
    p = plan
    nx, ny, nz, nzl = p.nx, p.ny, p.nz, p.nzl
    rows, half, block, own, taps = p.rows, p.half, p.block, p.own, p.taps
    pairs = rows // 2
    seq, batch = lax.axis_index("seq"), lax.axis_index("batch")
    core = seq % 2
    x = (seq // 2) % nx
    z_lo = seq // (2 * nx)
    z_hi = batch % p.nzh
    y = batch // p.nzh
    z = z_hi * nzl + z_lo
    sign = 1 - 2 * core
    other = 1 - core

    def device(zz, xx, cc, yy):
        return ((zz % nzl) * (2 * nx) + xx * 2 + cc, yy * p.nzh + zz // nzl)

    def at_z(d):
        return (z + d + nz) % nz

    def at_x(d):
        return (x + d) % nx

    def at_y(d):
        return (y + d) % ny

    chip = z * nx + x
    chips = nz * nx
    nxt = (chip + 1) % chips
    prv = (chip + chips - 1) % chips

    partner = device(z, x, other, y)

    def chip_core(c, cc):
        return device(c // nx, c % nx, cc, y)

    XFAR = sorted(range(1, nx), key=lambda d: -min(d, nx - d))
    YFAR = sorted(range(1, ny), key=lambda d: -min(d, ny - d))
    ZFAR = sorted(range(1, nz), key=lambda d: -min(d, nz - d))
    SQUARE = sorted(
        ((dy, dx) for dy in range(ny) for dx in range(nx)), key=lambda v: -min(v[0], ny - v[0]) - min(v[1], nx - v[1])
    )
    barrier = pltpu.get_barrier_semaphore()
    peers = [partner]
    peers += [device(z, at_x(d), cc, y) for d in range(1, nx) for cc in (core, other)]
    peers += [device(z, x, core, at_y(d)) for d in range(1, ny)]
    far = nzl // 2
    near = min(2, far)
    peers += [device(at_z(s * o), x, core, y) for o in range(1, near + 1) for s in (1, -1)]
    peers += [chip_core(c, cc) for c in (nxt, prv) for cc in (0, 1)]
    for peer in peers:
        pl.semaphore_signal(barrier, inc=1, device_id=peer, device_id_type=MESH)

    loads = [
        pltpu.make_async_copy(src, dst, s_in.at[i])
        for i, (src, dst) in enumerate(
            ((activ_h.at[0], activ.at[0]), (gain_h, gain), (weight_h, weight), (bias_h, bias), (cot_h_.at[0], cot.at[0]))
        )
    ]
    for load in loads:
        load.start()
    q = lax.broadcasted_iota(jnp.int32, (8, p.halfp), 1)
    chan = own * ((q % block) // own * (2 * nx) + (q // block) * 2) + q % own
    chan = jnp.where(q < half, chan, 2 * p.cin)[0:1]
    r = lax.broadcasted_iota(jnp.int32, (p.cin, p.halfp), 0)
    sel[0] = jnp.where(r == chan, 1.0, 0.0).astype(BF16)
    sel[1] = jnp.where(r == chan + own, 1.0, 0.0).astype(BF16)
    mine = sel[core]

    ct[...] = jnp.zeros_like(ct)
    for load in loads:
        load.wait()
    tiles = p.halfp // 128

    def put(start, value):
        for t in range(tiles):
            af[t, pl.ds(start, value.shape[0]), :] = value[:, 128 * t:128 * t + 128]

    put(pl.multiple_of(PAD + rows * core, 8), dot(activ[0], mine, NN))
    ct[pl.ds(pl.multiple_of(PAD + pairs * core, 8), pairs), 0:p.cout] = cot[0].astype(F32)
    gain_half = picked(gain[...].reshape(1, p.cin), mine, NN)

    pl.semaphore_wait(barrier, len(peers))

    for s in (1, -1):
        pl.semaphore_signal(far_sem, inc=1, device_id=device(at_z(s * near), x, core, y), device_id_type=MESH)

    started = []

    def send(src, dst, s, r_, to):
        copy = pltpu.make_async_remote_copy(
            src_ref=src, dst_ref=dst, send_sem=s, recv_sem=r_, device_id=to, device_id_type=MESH
        )
        copy.start()
        started.append(copy)
        return copy

    def share(src, dst, s, r_, to):
        pltpu.make_async_remote_copy(
            src_ref=src, dst_ref=dst, send_sem=s, recv_sem=r_, device_id=to, device_id_type=MESH
        ).start()

    def whole(region, sem):
        return pltpu.make_async_remote_copy(
            src_ref=region, dst_ref=region, send_sem=sem, recv_sem=sem, device_id=partner, device_id_type=MESH
        )

    def arrived(region, sem):
        whole(region, sem).wait_recv()

    c_act = send(activ.at[0], act_p, s_loc.at[0], r_loc.at[0], partner)
    c_cot = send(cot.at[0], cot_p, s_loc.at[1], r_loc.at[1], partner)
    edge = 16
    up_chip = jnp.where(core == 1, nxt, prv)
    side = core
    halos = []
    a_edge = pl.ds(pl.multiple_of(core * (rows - edge), edge), edge)
    c_edge = pl.ds(pl.multiple_of(core * (pairs - edge), edge), edge)
    for i, cc in enumerate((0, 1)):
        to = chip_core(up_chip, cc)
        halos.append(send(activ.at[0, a_edge], act_h.at[side], s_loc.at[2 + i], r_loc.at[2 + side], to))
        halos.append(send(cot.at[0, c_edge], cot_h.at[side], s_loc.at[4 + i], r_loc.at[4 + side], to))
    n_off = len(p.offsets)
    c_az = []
    for n, k in enumerate(VIA_Z):
        for d in XFAR:
            share(weight.at[k], xb.at[n, x], s_xf.at[0], r_xf.at[n], device(z, at_x(d), core, y))
        xb[n, x] = weight[k]
    direct = range(taps - len(VIA_Z))

    def weights_out(wanted):
        for k in direct:
            for o in sorted(p.offsets, key=lambda v: -abs(v)):
                if (abs(o) <= near) == wanted:
                    to = device(at_z(sign * o), x, core, y)
                    share(weight.at[k], zb.at[z_lo, k], s_az.at[0], r_az.at[k], to)

    weights_out(True)
    zb[z_lo] = weight[...]

    def activate(start, count):
        for t in range(tiles):
            v = af[t, start:start + count, :] * gain_half[:, 128 * t:128 * t + 128]
            gf[t, start:start + count, :] = (
                0.5 * v * (1.0 + jnp.tanh(ROOT * (v + CUBE * v * v * v)))
            ).astype(BF16).astype(F32)

    def strided(ref, start):
        return jnp.concatenate([ref[t, pl.ds(start, rows, 2), :] for t in range(tiles)], axis=1)

    def cot_shift(d):
        return ct[PAD + d:PAD + d + rows, :].astype(BF16)

    def y_send(k, part):
        for t in range(ny):
            dwo[t, k] = part[:, 128 * t:128 * t + 128]
            dws[t, k] = part[:, 128 * t:128 * t + 128].astype(BF16)
        for d in YFAR:
            share(dws.at[at_y(d), k], yr.at[k, d - 1], s_y.at[0], r_y.at[k], device(z, x, core, at_y(d)))

    c_act.wait_recv()
    put(pl.multiple_of(PAD + rows * other, 8), dot(act_p[...], mine, NN))
    c_cot.wait_recv()
    ct[pl.ds(pl.multiple_of(PAD + pairs * other, 8), pairs), 0:p.cout] = cot_p[...].astype(F32)
    bias_part = jnp.sum(ct[PAD:PAD + rows, :], axis=0, keepdims=True)
    for t in range(ny):
        bt[t:t + 1, :] = bias_part[:, 128 * t:128 * t + 128]

    for d in YFAR:
        share(bt, bx.at[d - 1], s_bx.at[0], r_bx.at[0], device(z, x, core, at_y(d)))

    def bias_x(_):
        arrived(bx.at[pl.ds(0, ny - 1)], r_bx.at[0])
        total = bt[...]
        for i in range(ny - 1):
            total = total + bx[i]
        bu[...] = total
        for d in XFAR:
            share(bu, bx.at[ny - 2 + d], s_bx.at[1], r_bx.at[1], device(z, at_x(d), core, y))

    def bias_sum(_):
        arrived(bx.at[pl.ds(ny - 1, nx - 1)], r_bx.at[1])
        total = bu[...]
        for i in range(nx - 1):
            total = total + bx[ny - 1 + i]
        bs[...] = total
        for d in ZFAR:
            share(bs, bz.at[d - 1], s_bz.at[0], r_bz.at[0], device(at_z(d), x, core, y))

    activate(PAD, 2 * rows)
    even, odd = strided(gf, PAD).astype(BF16), strided(gf, PAD + 1).astype(BF16)
    here = cot_shift(0)
    e0, o0 = dot(even, here, TN)[0:half], dot(odd, here, TN)[0:half]
    y_send(2, 0.5 * (e0 + o0))
    pl.semaphore_wait(far_sem, 2)
    weights_out(False)

    for s in (0, 1):
        for src, dst, i in ((activ.at[0, a_edge], act_h, 2), (cot.at[0, c_edge], cot_h, 4)):
            pltpu.make_async_remote_copy(
                src_ref=src, dst_ref=dst.at[s], send_sem=s_loc.at[i], recv_sem=r_loc.at[i + s],
                device_id=partner, device_id_type=MESH,
            ).wait_recv()
    place = z_lo * nx + x
    before = jnp.where(place > 0, 1.0, 0.0).astype(F32)
    after = jnp.where(place < nzl * nx - 1, 1.0, 0.0).astype(F32)
    ct[0:PAD, 0:p.cout] = (cot_h[1].astype(F32) * before)[edge - PAD:edge]
    ct[PAD + rows:, 0:p.cout] = (cot_h[0].astype(F32) * after)[0:PAD]
    up, down = cot_shift(1), cot_shift(-1)
    e_down = dot(even, down, TN)[0:half]
    part = 0.5 * (e_down + dot(odd, down, TN)[0:half])
    for xx in range(nx):
        fo[xx] = part[block * xx:block * (xx + 1)]
        fs[xx] = part[block * xx:block * (xx + 1)].astype(BF16)
    for d in XFAR:
        share(fs.at[at_x(d)], fr.at[d - 1], s_f.at[0], r_f.at[0], device(z, at_x(d), core, y))
    o_up = dot(odd, up, TN)[0:half]
    y_send(1, 0.5 * (e0 + o_up))
    y_send(3, 0.5 * (e_down + o0))
    y_send(0, 0.5 * (dot(even, up, TN)[0:half] + o_up))
    put(0, (dot(act_h[1], mine, NN) * before)[edge - PAD:edge])
    put(PAD + 2 * rows, (dot(act_h[0], mine, NN) * after)[0:PAD])
    activate(0, PAD)
    activate(PAD + 2 * rows, PAD)

    def weights_z(k):
        arrived(zb.at[pl.ds(0, n_off), k], r_az.at[k])
        for zz in range(nzl):
            wf[k % 2, own * zz:own * (zz + 1)] = zb[zz, k].astype(F32)
        wx[x, k] = wf[k % 2].astype(BF16)
        for d in XFAR:
            share(wx.at[x, k], wx.at[x, k], s_ax.at[0], r_ax.at[k], device(z, at_x(d), core, y))

    def weights_x(n):
        arrived(xb.at[n, pl.ds(0, nx - 1)], r_xf.at[n])
        for xx in range(nx):
            wg[n, own * xx:own * (xx + 1)] = xb[n, xx].astype(F32)
        xp[n] = wg[n].astype(BF16)
        for o in sorted(p.offsets, key=lambda v: -abs(v)):
            share(xp.at[n], zx.at[n, z_lo], s_zf.at[0], r_zf.at[n], device(at_z(sign * o), x, core, y))
        zx[n, z_lo] = xp[n]

    def weights_last(n):
        arrived(zx.at[n, pl.ds(0, n_off)], r_zf.at[n])
        for zz in range(nzl):
            rows_z = zx[n, zz].astype(F32)
            for xx in range(nx):
                wh[xx, own * zz:own * (zz + 1)] = rows_z[own * xx:own * (xx + 1)]
        for xx in range(nx):
            wx[xx, VIA_Z[n]] = wh[xx].astype(BF16)

    def y_sum(n):
        k = TAPS[n]
        arrived(yr.at[k], r_y.at[k])
        total = dwo[y, k]
        for d in range(ny - 1):
            total = total + yr[k, d].astype(F32)
        for xx in range(nx):
            piece = total[block * xx:block * (xx + 1)]
            xo[xx, k] = piece
            xs[xx, k] = piece.astype(BF16)
        for d in XFAR:
            share(xs.at[at_x(d), k], xr.at[k, d - 1], s_x.at[0], r_x.at[k], device(z, at_x(d), core, y))

    def x_first(_):
        arrived(fr, r_f.at[0])
        total = fo[x]
        for d in range(nx - 1):
            total = total + fr[d].astype(F32)
        for t in range(ny):
            go[t] = total[:, 128 * t:128 * t + 128]
            gb[t] = total[:, 128 * t:128 * t + 128].astype(BF16)
        for d in YFAR:
            share(gb.at[at_y(d)], gr.at[d - 1], s_g.at[0], r_g.at[0], device(z, x, core, at_y(d)))

    z_s, z_r = (zs0, zs1), (zr0, zr1)
    def x_sum(g):
        base, length, members = GROUPS[g]
        zo[:, base:base + length, :] = jnp.zeros((nzl, length, 128), F32)
        for n, k in enumerate(members):
            if k == X_FIRST:
                arrived(gr, r_g.at[0])
            else:
                arrived(xr.at[k], r_x.at[k])
            total = go[y] if k == X_FIRST else xo[x, k]
            for d in range((ny if k == X_FIRST else nx) - 1):
                total = total + (gr[d] if k == X_FIRST else xr[k, d]).astype(F32)
            for zz in range(nzl):
                zo[zz, base + own * n:base + own * (n + 1), :] = total[own * zz:own * (zz + 1)]
        z_s[g][...] = zo[:, base:base + length, :].astype(BF16)
        for d in ZFAR:
            share(z_s[g].at[at_z(d) % nzl], z_r[g].at[d - 1], s_z.at[g], r_z.at[g], device(at_z(d), x, core, y))

    acc = [None]
    cot_all = ct[:, 0:p.cout].astype(BF16)
    shifted = [strided(gf, PAD - 2 + j)[:, 0:half].astype(BF16) for j in range(taps + 1)]

    def convs(k):
        if k not in VIA_Z:
            arrived(wx.at[pl.ds(0, nx - 1), k], r_ax.at[k])
        w = wx[:, k].reshape(half, p.cout)
        add = dot(shifted[k], w, NN) + dot(shifted[k + 1], w, NN)
        acc[0] = add if acc[0] is None else acc[0] + add
        cks[k, :, 0:half] = dot(cot_all, w, NT)
        if half < p.halfp:
            cks[k, :, half:] = jnp.zeros((rows + 2 * PAD, p.halfp - half), F32)

    for step, k in ORDER:
        {"wz": weights_z, "ys": y_sum, "cv": convs, "xs": x_sum, "xf": weights_x, "zf": weights_last, "x1": x_first, "bx": bias_x, "bs": bias_sum}[step](k)
    conv = acc[0]
    conv = 0.5 * conv
    for h in (0, 1):
        pf_s[h] = conv[pairs * h:pairs * (h + 1)]
    c_pf = send(pf_s.at[other], pf_r, s_loc.at[6], r_loc.at[6], partner)

    def shift(k, d):
        return cks[k, PAD + d:PAD + d + rows, :]

    grad_even = 0.5 * (shift(0, 1) + shift(1, 0) + shift(2, 0) + shift(3, -1) + shift(4, -1))
    grad_odd = 0.5 * (shift(0, 1) + shift(1, 1) + shift(2, 0) + shift(3, 0) + shift(4, -1))
    gain_part = jnp.zeros((1, p.halfp), F32)
    for start, grad in ((0, grad_even), (1, grad_odd)):
        a = strided(af, PAD + start)
        v = a * gain_half
        t = jnp.tanh(ROOT * (v + CUBE * v * v * v))
        slope = 0.5 * (1.0 + t) + 0.5 * v * (1.0 - t * t) * (ROOT * (1.0 + 3.0 * CUBE * v * v))
        pre = grad * slope
        gain_part = gain_part + jnp.sum(pre * a, axis=0, keepdims=True)
        out = pre * gain_half
        for tt in range(p.halfp // 128):
            io[tt, pl.ds(start, rows, 2), :] = out[:, 128 * tt:128 * tt + 128]
    for h in (0, 1):
        gi_s[h] = jnp.concatenate(
            [io[tt, rows * h:rows * (h + 1), :] for tt in range(p.halfp // 128)], axis=1
        ).astype(BF16)
    c_gi = send(gi_s.at[other], gi_r, s_loc.at[7], r_loc.at[7], partner)

    for t in range(tiles):
        gt[0, t:t + 1, :] = gain_part[:, 128 * t:128 * t + 128]
    for dy, dx in SQUARE:
        for flip in (0, 1):
            i = (flip * ny + dy) * nx + dx
            if i > 0:
                cc = core if flip == 0 else other
                share(gt.at[0], gx.at[i], s_gx.at[0], r_gx.at[0], device(z, at_x(dx), cc, at_y(dy)))

    for g in LATE:
        x_sum(g)

    others = gx.at[pl.ds(1, 2 * nx * ny - 1)]
    arrived(others, r_gx.at[0])
    same = gt[0]
    for i in range(1, ny * nx):
        same = same + gx[i]
    flipped = gx[ny * nx]
    for i in range(1, ny * nx):
        flipped = flipped + gx[ny * nx + i]
    first = jnp.where(core == 0, same, flipped)
    second = jnp.where(core == 0, flipped, same)
    gs[0:tiles, :] = first
    gs[tiles:2 * tiles, :] = second
    for d in ZFAR:
        share(gs, gz.at[d - 1], s_gz.at[0], r_gz.at[0], device(at_z(d), x, core, y))

    c_pf.wait_recv()
    pooled[0] = (pf_s[core] + pf_r[...] + bias[...].reshape(1, p.cout)).astype(BF16)
    c_gi.wait_recv()
    grad_input[0] = (dot(gi_s[core], mine, NT) + dot(gi_r[...], sel[other], NT)).astype(BF16)

    for g in range(len(GROUPS)):
        arrived(z_r[g], r_z.at[g])
    for g, (base, length, members) in enumerate(GROUPS):
        final = zo[z_lo, base:base + length, :]
        for d in range(nz - 1):
            final = final + z_r[g][d].astype(F32)
        ya[y, base:base + length, :] = final * factor
    c_ya = []
    for d in range(1, ny):
        c_ya.append(send(ya.at[y], ya.at[y], s_ya.at[d - 1], r_ya.at[d - 1], device(z, x, core, at_y(d))))

    arrived(gz, r_gz.at[0])
    total = gs[...]
    for d in range(nz - 1):
        total = total + gz[d]
    total = total * factor
    halves = [
        jnp.concatenate([total[tiles * h + t:tiles * h + t + 1] for t in range(tiles)], axis=1) for h in (0, 1)
    ]
    grad_gain[...] = (picked(halves[0], sel[0], NT) + picked(halves[1], sel[1], NT)).reshape(p.cin)

    arrived(bz, r_bz.at[0])
    total = bs[...]
    for d in range(nz - 1):
        total = total + bz[d]
    total = total * factor
    grad_bias[...] = jnp.concatenate([total[t:t + 1] for t in range(ny)], axis=1)[:, 0:p.cout].reshape(p.cout)

    for c in c_ya:
        c.wait_recv()
    for base, length, members in GROUPS:
        for n, k in enumerate(members):
            row = base + own * n
            wide = jnp.concatenate([ya[t, row:row + own, :] for t in range(ny)], axis=1)
            grad_weight[k] = wide[:, 0:p.cout]
    for c in started:
        c.wait_send()
    n_direct, n_via, n_y = len(direct), len(VIA_Z), len(TAPS)
    for region, sem in (
        (xb.at[:, pl.ds(0, nx - 1)], s_xf), (zb.at[pl.ds(0, n_off), pl.ds(0, n_direct)], s_az), (yr, s_y),
        (bz, s_bz), (fr, s_f), (gr, s_g), (wx.at[pl.ds(0, nx - 1), pl.ds(0, n_direct)], s_ax),
        (zx.at[:, pl.ds(0, n_off)], s_zf), (xr, s_x), (others, s_gx), (gz, s_gz),
    ):
        whole(region, sem.at[0]).wait_send()
    for g in range(len(GROUPS)):
        whole(z_r[g], s_z.at[g]).wait_send()
    whole(bx.at[pl.ds(0, ny - 1)], s_bx.at[0]).wait_send()
    whole(bx.at[pl.ds(ny - 1, nx - 1)], s_bx.at[1]).wait_send()


def hand_over(*refs):
    for src, dst in zip(refs[:5], refs[5:]):
        dst[...] = src[...]


def build(mesh, plan, factor):
    p = plan
    nx, ny, nz, nzl = p.nx, p.ny, p.nz, p.nzl
    pairs = p.rows // 2
    zrows = sum(length for _, length, _ in GROUPS)
    dma = pltpu.SemaphoreType.DMA
    n_direct, n_via, n_y = p.taps - len(VIA_Z), len(VIA_Z), len(TAPS)
    sems = (
        (8, 8), (1, n_direct), (1, n_direct), (1, n_y), (1, n_y), (len(GROUPS),) * 2, (ny - 1, ny - 1),
        (1, 1), (1, 1), (1, n_via), (1, n_via), (2, 2), (1, 1), (1, 1), (1, 1),
    )
    scratch = [
        pltpu.VMEM((1, p.rows, p.cin), BF16),
        pltpu.VMEM((p.cin,), F32),
        pltpu.VMEM((p.taps, p.own, p.cout), BF16),
        pltpu.VMEM((p.cout,), F32),
        pltpu.VMEM((1, pairs, p.cout), BF16),
        dma((5,)),
        pltpu.SemaphoreType.REGULAR,
        pltpu.VMEM((p.rows, p.cin), BF16),
        pltpu.VMEM((pairs, p.cout), BF16),
        pltpu.VMEM((2, 16, p.cin), BF16),
        pltpu.VMEM((2, 16, p.cout), BF16),
        pltpu.VMEM((2, p.cin, p.halfp), BF16),
        pltpu.VMEM((p.halfp // 128, 2 * p.rows + 2 * PAD, 128), F32),
        pltpu.VMEM((p.halfp // 128, 2 * p.rows + 2 * PAD, 128), F32),
        pltpu.VMEM((p.rows + 2 * PAD, p.coutp), F32),
        pltpu.VMEM((nzl, p.taps, p.own, p.cout), BF16),
        pltpu.VMEM((2, p.block, p.cout), F32),
        pltpu.VMEM((nx, p.taps, p.block, p.cout), BF16),
        pltpu.VMEM((ny, p.taps, p.half, 128), BF16),
        pltpu.VMEM((ny, p.taps, p.half, 128), F32),
        pltpu.VMEM((len(TAPS), ny - 1, p.half, 128), BF16),
        pltpu.VMEM((nx, p.taps, p.block, 128), BF16),
        pltpu.VMEM((nx, p.taps, p.block, 128), F32),
        pltpu.VMEM((len(TAPS), nx - 1, p.block, 128), BF16),
        pltpu.VMEM((nzl, zrows, 128), F32),
        *[pltpu.VMEM((nzl, length, 128), BF16) for _, length, _ in GROUPS],
        *[pltpu.VMEM((nz - 1, length, 128), BF16) for _, length, _ in GROUPS],
        pltpu.VMEM((ny, zrows, 128), F32),
        pltpu.VMEM((len(VIA_Z), nx, p.own, p.cout), BF16),
        pltpu.VMEM((len(VIA_Z), p.own * nx, p.cout), BF16),
        pltpu.VMEM((len(VIA_Z), nzl, p.own * nx, p.cout), BF16),
        pltpu.VMEM((len(VIA_Z), p.own * nx, p.cout), F32),
        pltpu.VMEM((nx, p.block, p.cout), F32),
        pltpu.VMEM((p.taps, p.rows + 2 * PAD, p.halfp), F32),
        pltpu.VMEM((p.halfp // 128, 2 * p.rows, 128), F32),
        pltpu.VMEM((2, p.rows, p.halfp), BF16),
        pltpu.VMEM((p.rows, p.halfp), BF16),
        pltpu.VMEM((2, pairs, p.cout), F32),
        pltpu.VMEM((pairs, p.cout), F32),
        pltpu.VMEM((2 * nx * ny, p.halfp // 128, 128), F32),
        pltpu.VMEM((1, p.halfp // 128, 128), F32),
        pltpu.VMEM((p.halfp // 64, 128), F32),
        pltpu.VMEM((nz - 1, p.halfp // 64, 128), F32),
        pltpu.VMEM((ny, 128), F32),
        pltpu.VMEM((ny, 128), F32),
        pltpu.VMEM((ny - 1 + nx - 1, ny, 128), F32),
        pltpu.VMEM((ny, 128), F32),
        pltpu.VMEM((nz - 1, ny, 128), F32),
        pltpu.VMEM((nx, p.block, p.coutp), F32),
        pltpu.VMEM((nx, p.block, p.coutp), BF16),
        pltpu.VMEM((nx - 1, p.block, p.coutp), BF16),
        pltpu.VMEM((ny, p.block, 128), F32),
        pltpu.VMEM((ny, p.block, 128), BF16),
        pltpu.VMEM((ny - 1, p.block, 128), BF16),
    ]
    for sent, received in sems:
        scratch += [dma((sent,)), dma((received,))]
    vmem = pl.BlockSpec(memory_space=pltpu.VMEM)

    hbm = pl.BlockSpec(memory_space=pltpu.HBM)
    shapes = (
        jax.ShapeDtypeStruct((1, pairs, p.cout), BF16),
        jax.ShapeDtypeStruct((1, p.rows, p.cin), BF16),
        jax.ShapeDtypeStruct((p.taps, p.own, p.cout), F32),
        jax.ShapeDtypeStruct((p.cin,), F32),
        jax.ShapeDtypeStruct((p.cout,), F32),
    )

    def per_device(activ, gain, weight, bias, cotangent):
        outs = pl.pallas_call(
            functools.partial(kernel, p, factor),
            out_shape=shapes,
            in_specs=[hbm] * 5,
            out_specs=(vmem,) * 5,
            scratch_shapes=scratch,
            compiler_params=pltpu.CompilerParams(collective_id=0, has_side_effects=True),
        )(activ, gain, weight, bias, cotangent)
        return pl.pallas_call(
            hand_over, out_shape=shapes, in_specs=[vmem] * 5, out_specs=(vmem,) * 5,
        )(*outs)

    in_specs = (P("batch", "seq", None), P(), P(None, "seq", None), P(), P("batch", "seq", None))
    out_specs = (P("batch", "seq", None), P("batch", "seq", None), P(None, "seq", None), P(), P())
    return jax.shard_map(per_device, mesh=mesh, in_specs=in_specs, out_specs=out_specs, check_vma=False)


def solution(mesh):
    return build(mesh, Plan(), float(8 * 8192) ** -0.5)
```
